16 devices in a mesh: dp: 2 (over z), tp: 8 (over y, x, core).
Axes of the slice: x: 2, y: 2, z: 2, core: 2. Of those that a mesh axis runs over, the one named last changes fastest.
Arguments:
- x: bfloat16 [1024, 2048], P('dp'), parts along dimension 0
- k_cache: bfloat16 [1024, 32, 16, 128], P('dp', None, 'tp'), parts along dimension 0
- v_cache: bfloat16 [1024, 32, 16, 128], P('dp', None, 'tp'), parts along dimension 0
- positions: int32 [1024], P('dp'), parts along dimension 0
- att_ids: int32 [1024, 2], P('dp'), parts along dimension 0
- mlp_ids: int32 [1024, 2], P('dp'), parts along dimension 0
- norm_att: float32 [2048], replicated
- w_kv: bfloat16 [2048, 16, 256], P(None, 'tp')
- router_att: bfloat16 [2048, 8], replicated
- w_query: bfloat16 [8, 2048, 2048], P(None, None, 'tp')
- w_out: bfloat16 [8, 2048, 2048], P(None, 'tp')
- norm_mlp: float32 [2048], replicated
- router_mlp: bfloat16 [2048, 8], replicated
- w_gate: bfloat16 [8, 2048, 5632], P('tp')
- w_up: bfloat16 [8, 2048, 5632], P('tp')
- w_down: bfloat16 [8, 5632, 2048], P('tp')
Outputs:
- output 1: bfloat16 [1024, 2048], P('dp'), parts along dimension 0
- output 2: bfloat16 [1024, 32, 16, 128], P('dp', None, 'tp'), parts along dimension 0
- output 3: bfloat16 [1024, 32, 16, 128], P('dp', None, 'tp'), parts along dimension 0
There are 2 independent parts. The reference program is written for one: setup_inputs(seed, part) draws one part's arguments, and reference() takes and returns one part's arrays. A program takes and returns all parts, laid end to end along the dimension named above; an argument that names none is the same for every part.
All inputs are finite; a program needn't handle non-finite values.
Results may differ from the reference program's by a relative error of at most 0.0127623.
Values are sent between devices in bfloat16 or wider.
A program may use at most 1 GiB of HBM per device.

```python
import jax
import jax.numpy as jnp
from jax import lax

HIDDEN = 2048
KV_HEADS = 16
HEAD_DIM = 128
ATT_EXPERTS = 8
MLP_EXPERTS = 8
FFN_WIDTH = 5632
TOKENS = 512
CACHE_LEN = 32

QUERY_WIDTH = KV_HEADS * HEAD_DIM
NORM_EPS = 1e-6
ROPE_BASE = 10000.0


def draw_pair(base_key, experts, skewed):
    key_first, key_offset, key_hot, key_share, key_coin = jax.random.split(base_key, 5)
    first_pick = jax.random.randint(key_first, (TOKENS,), 0, experts)
    if skewed:
        hot_id = jax.random.randint(key_hot, (), 0, experts)
        hot_share = jax.random.randint(key_share, (), 40, 61)
        coin_flip = jax.random.randint(key_coin, (TOKENS,), 0, 100)
        first_pick = jnp.where(coin_flip < hot_share, hot_id, first_pick)
    offset = jax.random.randint(key_offset, (TOKENS,), 1, experts)
    token_index = jnp.arange(TOKENS)
    forced = (token_index < experts) & (token_index != first_pick)
    second_pick = jnp.where(forced, token_index, (first_pick + offset) % experts)
    return jnp.stack([first_pick, second_pick], axis=1).astype(jnp.int32)


def draw_positions(base_key):
    positions = jax.random.randint(base_key, (TOKENS,), CACHE_LEN // 4, CACHE_LEN)
    return positions.at[0].set(CACHE_LEN - 1).at[1].set(CACHE_LEN // 4).astype(jnp.int32)


def setup_inputs(seed: int = 0, part: int = 0) -> dict:
    shared_keys = jax.random.split(jax.random.key(seed), 10)
    part_keys = jax.random.split(jax.random.fold_in(jax.random.key(seed + 1), part), 6)
    cache_shape = (TOKENS, CACHE_LEN, KV_HEADS, HEAD_DIM)
    x = jax.random.normal(part_keys[0], (TOKENS, HIDDEN), jnp.float32).astype(jnp.bfloat16)
    k_cache = jax.random.normal(part_keys[1], cache_shape, jnp.float32).astype(jnp.bfloat16)
    value_mean = jax.random.normal(part_keys[2], (TOKENS, 1, KV_HEADS, HEAD_DIM), jnp.float32)
    value_noise = jax.random.normal(part_keys[3], cache_shape, jnp.float32)
    v_cache = (0.8 * value_mean + 0.6 * value_noise).astype(jnp.bfloat16)
    positions = draw_positions(part_keys[4])
    choice_keys = jax.random.split(part_keys[5], 2)
    att_ids = draw_pair(choice_keys[0], ATT_EXPERTS, False)
    mlp_ids = draw_pair(choice_keys[1], MLP_EXPERTS, True)
    norm_att = 1.0 + 0.3 * jax.random.normal(shared_keys[0], (HIDDEN,), jnp.float32)
    w_kv = (jax.random.normal(shared_keys[1], (HIDDEN, KV_HEADS, 2 * HEAD_DIM), jnp.float32) * HIDDEN ** -0.5).astype(jnp.bfloat16)
    router_att = (jax.random.normal(shared_keys[2], (HIDDEN, ATT_EXPERTS), jnp.float32) * 0.5 * HIDDEN ** -0.5).astype(jnp.bfloat16)
    w_query = (jax.random.normal(shared_keys[3], (ATT_EXPERTS, HIDDEN, QUERY_WIDTH), jnp.float32) * HIDDEN ** -0.5).astype(jnp.bfloat16)
    w_out = (jax.random.normal(shared_keys[4], (ATT_EXPERTS, QUERY_WIDTH, HIDDEN), jnp.float32) * QUERY_WIDTH ** -0.5).astype(jnp.bfloat16)
    norm_mlp = 1.0 + 0.3 * jax.random.normal(shared_keys[5], (HIDDEN,), jnp.float32)
    router_mlp = (jax.random.normal(shared_keys[6], (HIDDEN, MLP_EXPERTS), jnp.float32) * 0.5 * HIDDEN ** -0.5).astype(jnp.bfloat16)
    w_gate = (jax.random.normal(shared_keys[7], (MLP_EXPERTS, HIDDEN, FFN_WIDTH), jnp.float32) * HIDDEN ** -0.5).astype(jnp.bfloat16)
    w_up = (jax.random.normal(shared_keys[8], (MLP_EXPERTS, HIDDEN, FFN_WIDTH), jnp.float32) * HIDDEN ** -0.5).astype(jnp.bfloat16)
    w_down = (jax.random.normal(shared_keys[9], (MLP_EXPERTS, FFN_WIDTH, HIDDEN), jnp.float32) * FFN_WIDTH ** -0.5).astype(jnp.bfloat16)
    return {'x': x, 'k_cache': k_cache, 'v_cache': v_cache, 'positions': positions, 'att_ids': att_ids, 'mlp_ids': mlp_ids, 'norm_att': norm_att, 'w_kv': w_kv, 'router_att': router_att, 'w_query': w_query, 'w_out': w_out, 'norm_mlp': norm_mlp, 'router_mlp': router_mlp, 'w_gate': w_gate, 'w_up': w_up, 'w_down': w_down}


def rms_norm(x, gain):
    values = x.astype(jnp.float32)
    inv_rms = lax.rsqrt(jnp.mean(values * values, axis=-1, keepdims=True) + NORM_EPS)
    return (values * inv_rms * gain).astype(jnp.bfloat16)


def rope_tables(positions):
    half_dim = HEAD_DIM // 2
    inv_freq = ROPE_BASE ** (-(jnp.arange(half_dim, dtype=jnp.float32) * 2.0 / HEAD_DIM))
    angles = positions.astype(jnp.float32)[:, None] * inv_freq[None, :]
    return jnp.cos(angles), jnp.sin(angles)


def apply_rope(vectors, cos_table, sin_table):
    half_dim = vectors.shape[-1] // 2
    first_half = vectors[..., :half_dim]
    second_half = vectors[..., half_dim:]
    return jnp.concatenate([first_half * cos_table - second_half * sin_table, second_half * cos_table + first_half * sin_table], axis=-1)


def reference(x, k_cache, v_cache, positions, att_ids, mlp_ids, norm_att, w_kv, router_att, w_query, w_out, norm_mlp, router_mlp, w_gate, w_up, w_down):
    hidden = rms_norm(x, norm_att)
    kv_new = jnp.dot(hidden, w_kv.reshape(HIDDEN, KV_HEADS * 2 * HEAD_DIM), preferred_element_type=jnp.float32).reshape(TOKENS, KV_HEADS, 2 * HEAD_DIM)
    cos_table, sin_table = rope_tables(positions)
    key_new = apply_rope(kv_new[:, :, :HEAD_DIM], cos_table[:, None, :], sin_table[:, None, :]).astype(jnp.bfloat16)
    value_new = kv_new[:, :, HEAD_DIM:].astype(jnp.bfloat16)
    slot_index = jnp.arange(CACHE_LEN)
    at_slot = (slot_index[None, :] == positions[:, None])[:, :, None, None]
    keys_all = jnp.where(at_slot, key_new[:, None, :, :], k_cache)
    values_all = jnp.where(at_slot, value_new[:, None, :, :], v_cache)
    att_logits = jnp.dot(hidden, router_att, preferred_element_type=jnp.float32)
    att_gates = jax.nn.softmax(jnp.take_along_axis(att_logits, att_ids, axis=1), axis=-1)
    query_all = jnp.einsum('bd,edc->bec', hidden.astype(jnp.float32), w_query.astype(jnp.float32))
    query_sel = jnp.take_along_axis(query_all, att_ids[:, :, None], axis=1).reshape(TOKENS, 2, KV_HEADS, HEAD_DIM)
    query_rot = apply_rope(query_sel, cos_table[:, None, None, :], sin_table[:, None, None, :]).astype(jnp.bfloat16)
    scores = jnp.einsum('bknd,bsnd->bkns', query_rot.astype(jnp.float32), keys_all.astype(jnp.float32)) * HEAD_DIM ** -0.5
    visible = (slot_index[None, :] <= positions[:, None])[:, None, None, :]
    weights = jax.nn.softmax(jnp.where(visible, scores, -1e30), axis=-1).astype(jnp.bfloat16)
    attended = jnp.einsum('bkns,bsnd->bknd', weights.astype(jnp.float32), values_all.astype(jnp.float32)).astype(jnp.bfloat16).reshape(TOKENS, 2, QUERY_WIDTH)
    att_onehot = (att_ids[:, :, None] == jnp.arange(ATT_EXPERTS)[None, None, :]).astype(jnp.float32)
    out_slots = jnp.einsum('bke,bkc->bec', att_onehot, attended.astype(jnp.float32))
    projected = jnp.einsum('bec,ecd->bed', out_slots, w_out.astype(jnp.float32))
    att_dense = jnp.einsum('bke,bk->be', att_onehot, att_gates)
    att_sum = jnp.einsum('be,bed->bd', att_dense, projected)
    x_mid = (x.astype(jnp.float32) + att_sum).astype(jnp.bfloat16)
    normed = rms_norm(x_mid, norm_mlp)
    mlp_logits = jnp.dot(normed, router_mlp, preferred_element_type=jnp.float32)
    mlp_gates = jax.nn.softmax(jnp.take_along_axis(mlp_logits, mlp_ids, axis=1), axis=-1)
    mlp_onehot = (mlp_ids[:, :, None] == jnp.arange(MLP_EXPERTS)[None, None, :]).astype(jnp.float32)
    mlp_dense = jnp.einsum('bke,bk->be', mlp_onehot, mlp_gates)

    def expert_step(running_sum, expert_inputs):
        gate_mat, up_mat, down_mat, weight_col = expert_inputs
        gate_val = jnp.dot(normed, gate_mat, preferred_element_type=jnp.float32)
        up_val = jnp.dot(normed, up_mat, preferred_element_type=jnp.float32)
        activation = (jax.nn.silu(gate_val) * up_val).astype(jnp.bfloat16)
        down_out = jnp.dot(activation, down_mat, preferred_element_type=jnp.float32)
        return running_sum + weight_col[:, None] * down_out, None

    mlp_sum, _ = lax.scan(expert_step, jnp.zeros((TOKENS, HIDDEN), jnp.float32), (w_gate, w_up, w_down, mlp_dense.T))
    x_out = (x_mid.astype(jnp.float32) + mlp_sum).astype(jnp.bfloat16)
    return x_out, keys_all, values_all
```

```python
import functools

import jax
import jax.numpy as jnp
from jax import lax
from jax.experimental import pallas as pl
from jax.experimental.pallas import tpu as pltpu
from jax.sharding import PartitionSpec as P

NORM_EPS = 1e-6
ROPE_BASE = 10000.0
F32 = jnp.float32
BF16 = jnp.bfloat16
MESH = pl.DeviceIdType.MESH
CHUNK = 32


def rope_tables(positions, head_dim):
    half_dim = head_dim // 2
    inv_freq = ROPE_BASE ** (-(jnp.arange(half_dim, dtype=F32) * 2.0 / head_dim))
    angles = positions.astype(F32)[:, None] * inv_freq[None, :]
    cos, sin = jnp.cos(angles), jnp.sin(angles)
    return jnp.concatenate([cos, cos], axis=1), jnp.concatenate([-sin, sin], axis=1)


def rms_rows(x_ref, norm_ref, out_ref, rows, step):
    @pl.loop(0, rows // step)
    def _(i):
        sl = pl.ds(pl.multiple_of(i * step, step), step)
        v = x_ref[sl, :].astype(F32)
        inv = lax.rsqrt(jnp.mean(v * v, axis=-1, keepdims=True) + NORM_EPS)
        out_ref[sl, :] = (v * inv * norm_ref[...]).astype(BF16)


def qa_kernel(pos_s, meta_ref, x_ref, norm_ref, wkv_ref, router_ref, cos_ref, sin_ref, wq_hbm, k_hbm, v_hbm,
              o_ref, gates_ref, kout_hbm, vout_hbm,
              h_s, wq_s, kbuf, vbuf, kn_s, vn_s, q_s, idb_s, posb_s, wq_sem, k_sem, v_sem, ko_sem, vo_sem):
    tokens = x_ref.shape[0]
    experts = wq_hbm.shape[0]
    chunks = tokens // CHUNK
    crow = CHUNK * 64
    for e in range(experts):
        pltpu.make_async_copy(wq_hbm.at[e], wq_s.at[e], wq_sem.at[e]).start()
    for c in range(chunks):
        sl = pl.ds(c * crow, crow)
        pltpu.make_async_copy(k_hbm.at[sl], kbuf.at[sl], k_sem.at[c]).start()
        pltpu.make_async_copy(v_hbm.at[sl], vbuf.at[sl], v_sem.at[c]).start()
    rms_rows(x_ref, norm_ref, h_s, tokens, 32)
    idb_s[0] = jnp.broadcast_to(meta_ref[:, 0:1], (tokens, 128))
    idb_s[1] = jnp.broadcast_to(meta_ref[:, 1:2], (tokens, 128))
    posb_s[...] = jnp.broadcast_to(meta_ref[:, 2:3], (tokens, 128))
    cos, sin = cos_ref[...], sin_ref[...]

    def rope(v):
        return v * cos + pltpu.roll(v, 64, 1) * sin

    h = h_s[...]
    kv = jnp.dot(h, wkv_ref[...], preferred_element_type=F32)
    for n in range(2):
        kn_s[n] = rope(kv[:, n * 128:(n + 1) * 128])
        vn_s[n] = kv[:, 256 + n * 128:256 + (n + 1) * 128]
    logits = jnp.dot(h, router_ref[...], preferred_element_type=F32)
    lane = lax.broadcasted_iota(jnp.int32, (tokens, 128), 1)
    hit0, hit1 = lane == idb_s[0], lane == idb_s[1]
    l0 = jnp.sum(jnp.where(hit0, logits, 0.0), axis=1, keepdims=True)
    l1 = jnp.sum(jnp.where(hit1, logits, 0.0), axis=1, keepdims=True)
    top = jnp.maximum(l0, l1)
    e0, e1 = jnp.exp(l0 - top), jnp.exp(l1 - top)
    inv = 1.0 / (e0 + e1)
    gates_ref[...] = jnp.where(hit0, e0 * inv, 0.0) + jnp.where(hit1, e1 * inv, 0.0)

    @pl.loop(0, experts)
    def _(e):
        pltpu.make_async_copy(wq_hbm.at[e], wq_s.at[e], wq_sem.at[e]).wait()
        q = jnp.dot(h_s[...], wq_s[e], preferred_element_type=F32)
        for k in range(2):
            hit = idb_s[k] == e
            for n in range(2):
                part = q[:, n * 128:(n + 1) * 128].reshape(tokens // 8, 8, 128)
                h3 = hit.reshape(tokens // 8, 8, 128)
                q_s[:, 2 * n + k] = jnp.where(h3, part, q_s[:, 2 * n + k])

    cos3, sin3 = cos.reshape(tokens // 8, 8, 128), sin.reshape(tokens // 8, 8, 128)
    for j in range(4):
        v = q_s[:, j]
        q_s[:, j] = v * cos3 + pltpu.roll(v, 64, 2) * sin3

    col = lax.broadcasted_iota(jnp.int32, (8, 512), 1)
    row = lax.broadcasted_iota(jnp.int32, (8, 512), 0)
    slot = (col % 64) // 2
    same0 = (col // 64 == row) & (col % 2 == 0)
    same1 = (col // 64 == row) & (col % 2 == 1)
    r16 = lax.broadcasted_iota(jnp.int32, (16, 128), 0)
    odd16, pair16 = r16 % 2 == 1, r16 // 2

    @pl.loop(0, chunks)
    def _(c):
        sl = pl.ds(pl.multiple_of(c * crow, crow), crow)
        pltpu.make_async_copy(k_hbm.at[sl], kbuf.at[sl], k_sem.at[c]).wait()
        pltpu.make_async_copy(v_hbm.at[sl], vbuf.at[sl], v_sem.at[c]).wait()
        for t in range(CHUNK):
            tok = c * CHUNK + t
            p = pos_s[tok]
            at = pl.ds(pl.multiple_of(tok * 64 + (p // 8) * 16, 16), 16)
            here = pair16 == p % 8
            for buf, new in ((kbuf, kn_s), (vbuf, vn_s)):
                a = jnp.broadcast_to(new[0, pl.ds(tok, 1), :], (16, 128))
                b = jnp.broadcast_to(new[1, pl.ds(tok, 1), :], (16, 128))
                buf[at, :] = jnp.where(here, jnp.where(odd16, b, a), buf[at, :].astype(F32)).astype(BF16)
        pltpu.make_async_copy(kbuf.at[sl], kout_hbm.at[sl], ko_sem.at[c]).start()
        pltpu.make_async_copy(vbuf.at[sl], vout_hbm.at[sl], vo_sem.at[c]).start()
        for s in range(CHUNK // 8):
            blk = c * (CHUNK // 8) + s
            bs = pl.ds(pl.multiple_of(blk * 512, 512), 512)
            ts = pl.ds(pl.multiple_of(blk * 8, 8), 8)
            q = q_s[blk].reshape(32, 128).astype(BF16)
            sc = lax.dot_general(q, kbuf[bs, :], (((1,), (1,)), ((), ())), preferred_element_type=F32)
            pos = jnp.concatenate([posb_s[ts, :]] * 4, axis=1)
            vis = slot <= pos
            mask = jnp.concatenate([vis & same0] * 2 + [vis & same1] * 2, axis=0)
            sc = jnp.where(mask, sc * 128 ** -0.5, -1e30)
            ex = jnp.exp(sc - jnp.max(sc, axis=1, keepdims=True))
            w = (ex * (1.0 / jnp.sum(ex, axis=1, keepdims=True))).astype(BF16)
            o = jnp.dot(w, vbuf[bs, :], preferred_element_type=F32)
            for k in range(2):
                for n in range(2):
                    o_ref[k, ts, n * 128:(n + 1) * 128] = o[(2 * n + k) * 8:(2 * n + k + 1) * 8]

    @pl.loop(0, chunks)
    def _(c):
        sl = pl.ds(pl.multiple_of(c * crow, crow), crow)
        pltpu.make_async_copy(kbuf.at[sl], kout_hbm.at[sl], ko_sem.at[c]).wait()
        pltpu.make_async_copy(vbuf.at[sl], vout_hbm.at[sl], vo_sem.at[c]).wait()


def attention(pos, meta, x, norm, wkv, router, cos, sin, wq, kc, vc):
    tokens, width = x.shape
    experts, _, qw = wq.shape
    vmem = pl.BlockSpec(memory_space=pltpu.VMEM)
    hbm = pl.BlockSpec(memory_space=pl.ANY)
    chunks = tokens // CHUNK
    return pl.pallas_call(
        qa_kernel,
        name="qkv_attention",
        out_shape=(jax.ShapeDtypeStruct((2, tokens, qw), F32), jax.ShapeDtypeStruct((tokens, 128), F32),
                   jax.ShapeDtypeStruct(kc.shape, BF16), jax.ShapeDtypeStruct(vc.shape, BF16)),
        in_specs=[pl.BlockSpec(memory_space=pltpu.SMEM)] + [vmem] * 7 + [hbm] * 3,
        out_specs=(vmem, vmem, hbm, hbm),
        scratch_shapes=[
            pltpu.VMEM((tokens, width), BF16), pltpu.VMEM(wq.shape, BF16),
            pltpu.VMEM(kc.shape, BF16), pltpu.VMEM(vc.shape, BF16),
            pltpu.VMEM((2, tokens, 128), F32), pltpu.VMEM((2, tokens, 128), F32),
            pltpu.VMEM((tokens // 8, 4, 8, 128), F32), pltpu.VMEM((2, tokens, 128), jnp.int32),
            pltpu.VMEM((tokens, 128), jnp.int32),
            pltpu.SemaphoreType.DMA((experts,))] + [pltpu.SemaphoreType.DMA((chunks,))] * 4,
        compiler_params=pltpu.CompilerParams(vmem_limit_bytes=60 * 2**20),
    )(pos, meta, x, norm, wkv, router, cos, sin, wq, kc, vc)


def route_weights(logits, choice_ids, first_id, count):
    expert_index = first_id + jnp.arange(count)
    all_ids = jnp.arange(logits.shape[1])
    picked = jnp.sum(jnp.where(choice_ids[:, :, None] == all_ids[None, None, :], logits[:, None, :], 0.0), axis=2)
    pair_gates = jax.nn.softmax(picked, axis=-1)
    onehot = (choice_ids[:, :, None] == expert_index[None, None, :]).astype(F32)
    return jnp.sum(onehot * pair_gates[:, :, None], axis=1)


def rms_norm(x, gain):
    values = x.astype(F32)
    inv_rms = lax.rsqrt(jnp.mean(values * values, axis=-1, keepdims=True) + NORM_EPS)
    return (values * inv_rms * gain).astype(BF16)


def expert_part(normed, mlp_dense, w_gate, w_up, w_down):
    gate_val = jnp.einsum('bd,edf->bef', normed, w_gate, preferred_element_type=F32)
    up_val = jnp.einsum('bd,edf->bef', normed, w_up, preferred_element_type=F32)
    activation = (jax.nn.silu(gate_val) * up_val).astype(BF16)
    down_out = jnp.einsum('bef,efd->bed', activation, w_down, preferred_element_type=F32)
    return jnp.sum(mlp_dense[:, :, None] * down_out, axis=1)


def solution(mesh):
    def local_step(x, k_cache, v_cache, positions, att_ids, mlp_ids, norm_att, w_kv, router_att, w_query, w_out, norm_mlp, router_mlp, w_gate, w_up, w_down):
        tokens, width = x.shape
        cache_shape = k_cache.shape
        heads, head_dim = cache_shape[2], cache_shape[3]
        cos, sin = rope_tables(positions, head_dim)
        meta = jnp.concatenate([att_ids, positions[:, None]], axis=1)
        wkv = w_kv.reshape(width, heads, 2, head_dim).transpose(0, 2, 1, 3).reshape(width, 2 * heads * head_dim)
        router = jnp.pad(router_att, ((0, 0), (0, 128 - router_att.shape[1])))
        att, gates, keys_all, values_all = attention(
            positions, meta, x, norm_att[None, :], wkv, router, cos, sin, w_query,
            k_cache.reshape(-1, head_dim), v_cache.reshape(-1, head_dim))
        att = att.astype(BF16)
        slots = [jnp.where(att_ids[:, 0:1] == e, att[0], jnp.where(att_ids[:, 1:2] == e, att[1], 0)).astype(BF16) for e in range(8)]
        projected = jnp.einsum('ebc,ecd->bed', jnp.stack(slots), w_out, preferred_element_type=F32)
        att_part = jnp.sum(gates[:, :8, None] * projected, axis=1)
        att_sum = lax.psum(att_part.astype(BF16), 'tp').astype(F32)
        x_mid = (x.astype(F32) + att_sum).astype(BF16)
        normed = rms_norm(x_mid, norm_mlp)
        mlp_logits = jnp.dot(normed, router_mlp, preferred_element_type=F32)
        local_count = w_gate.shape[0]
        mlp_dense = route_weights(mlp_logits, mlp_ids, lax.axis_index('tp') * local_count, local_count)
        mlp_part = expert_part(normed, mlp_dense, w_gate, w_up, w_down)
        mlp_sum = lax.psum(mlp_part.astype(BF16), 'tp').astype(F32)
        x_out = (x_mid.astype(F32) + mlp_sum).astype(BF16)
        return x_out, keys_all.reshape(cache_shape), values_all.reshape(cache_shape)

    token_spec = P('dp', None)
    cache_spec = P('dp', None, 'tp', None)
    expert_spec = P('tp', None, None)
    in_specs = (token_spec, cache_spec, cache_spec, P('dp'), token_spec, token_spec, P(), P(None, 'tp', None), P(), P(None, None, 'tp'), P(None, 'tp', None), P(), P(), expert_spec, expert_spec, expert_spec)
    out_specs = (token_spec, cache_spec, cache_spec)
    return jax.shard_map(local_step, mesh=mesh, in_specs=in_specs, out_specs=out_specs, check_vma=False)
```

```python
import functools

import jax
import jax.numpy as jnp
from jax import lax
from jax.experimental import pallas as pl
from jax.experimental.pallas import tpu as pltpu
from jax.sharding import PartitionSpec as P

NORM_EPS = 1e-6
ROPE_BASE = 10000.0
F32 = jnp.float32
BF16 = jnp.bfloat16
MESH = pl.DeviceIdType.MESH
CHUNK = 32


def rope_tables(positions, head_dim):
    half_dim = head_dim // 2
    inv_freq = ROPE_BASE ** (-(jnp.arange(half_dim, dtype=F32) * 2.0 / head_dim))
    angles = positions.astype(F32)[:, None] * inv_freq[None, :]
    cos, sin = jnp.cos(angles), jnp.sin(angles)
    return jnp.concatenate([cos, cos], axis=1), jnp.concatenate([-sin, sin], axis=1)


def rms_rows(x_ref, norm_ref, out_ref, rows, step):
    @pl.loop(0, rows // step)
    def _(i):
        sl = pl.ds(pl.multiple_of(i * step, step), step)
        v = x_ref[sl, :].astype(F32)
        inv = lax.rsqrt(jnp.mean(v * v, axis=-1, keepdims=True) + NORM_EPS)
        out_ref[sl, :] = (v * inv * norm_ref[...]).astype(BF16)


def qa_kernel(pos_s, meta_ref, x_ref, norm_ref, wkv_ref, router_ref, cos_ref, sin_ref, wq_hbm, k_hbm, v_hbm,
              o_ref, gates_ref, kout_hbm, vout_hbm,
              h_s, wq_s, kbuf, vbuf, kn_s, vn_s, q_s, idb_s, posb_s, wq_sem, k_sem, v_sem, ko_sem, vo_sem):
    tokens = x_ref.shape[0]
    experts = wq_hbm.shape[0]
    chunks = tokens // CHUNK
    crow = CHUNK * 64
    for e in range(experts):
        pltpu.make_async_copy(wq_hbm.at[e], wq_s.at[e], wq_sem.at[e]).start()
    for c in range(chunks):
        sl = pl.ds(c * crow, crow)
        pltpu.make_async_copy(k_hbm.at[sl], kbuf.at[sl], k_sem.at[c]).start()
        pltpu.make_async_copy(v_hbm.at[sl], vbuf.at[sl], v_sem.at[c]).start()
    rms_rows(x_ref, norm_ref, h_s, tokens, 32)
    idb_s[0] = jnp.broadcast_to(meta_ref[:, 0:1], (tokens, 128))
    idb_s[1] = jnp.broadcast_to(meta_ref[:, 1:2], (tokens, 128))
    posb_s[...] = jnp.broadcast_to(meta_ref[:, 2:3], (tokens, 128))
    cos, sin = cos_ref[...], sin_ref[...]

    def rope(v):
        return v * cos + pltpu.roll(v, 64, 1) * sin

    h = h_s[...]
    kv = jnp.dot(h, wkv_ref[...], preferred_element_type=F32)
    for n in range(2):
        kn_s[n] = rope(kv[:, n * 128:(n + 1) * 128])
        vn_s[n] = kv[:, 256 + n * 128:256 + (n + 1) * 128]
    logits = jnp.dot(h, router_ref[...], preferred_element_type=F32)
    lane = lax.broadcasted_iota(jnp.int32, (tokens, 128), 1)
    hit0, hit1 = lane == idb_s[0], lane == idb_s[1]
    l0 = jnp.sum(jnp.where(hit0, logits, 0.0), axis=1, keepdims=True)
    l1 = jnp.sum(jnp.where(hit1, logits, 0.0), axis=1, keepdims=True)
    top = jnp.maximum(l0, l1)
    e0, e1 = jnp.exp(l0 - top), jnp.exp(l1 - top)
    inv = 1.0 / (e0 + e1)
    gates_ref[...] = jnp.where(hit0, e0 * inv, 0.0) + jnp.where(hit1, e1 * inv, 0.0)

    @pl.loop(0, experts)
    def _(e):
        pltpu.make_async_copy(wq_hbm.at[e], wq_s.at[e], wq_sem.at[e]).wait()
        q = jnp.dot(h_s[...], wq_s[e], preferred_element_type=F32)
        for k in range(2):
            hit = idb_s[k] == e
            for n in range(2):
                part = q[:, n * 128:(n + 1) * 128].reshape(tokens // 8, 8, 128)
                h3 = hit.reshape(tokens // 8, 8, 128)
                q_s[:, 2 * n + k] = jnp.where(h3, part, q_s[:, 2 * n + k])

    cos3, sin3 = cos.reshape(tokens // 8, 8, 128), sin.reshape(tokens // 8, 8, 128)
    for j in range(4):
        v = q_s[:, j]
        q_s[:, j] = v * cos3 + pltpu.roll(v, 64, 2) * sin3

    col = lax.broadcasted_iota(jnp.int32, (8, 512), 1)
    row = lax.broadcasted_iota(jnp.int32, (8, 512), 0)
    slot = (col % 64) // 2
    same0 = (col // 64 == row) & (col % 2 == 0)
    same1 = (col // 64 == row) & (col % 2 == 1)
    r16 = lax.broadcasted_iota(jnp.int32, (16, 128), 0)
    odd16, pair16 = r16 % 2 == 1, r16 // 2

    @pl.loop(0, chunks)
    def _(c):
        sl = pl.ds(pl.multiple_of(c * crow, crow), crow)
        pltpu.make_async_copy(k_hbm.at[sl], kbuf.at[sl], k_sem.at[c]).wait()
        pltpu.make_async_copy(v_hbm.at[sl], vbuf.at[sl], v_sem.at[c]).wait()
        for t in range(CHUNK):
            tok = c * CHUNK + t
            p = pos_s[tok]
            at = pl.ds(pl.multiple_of(tok * 64 + (p // 8) * 16, 16), 16)
            here = pair16 == p % 8
            for buf, new in ((kbuf, kn_s), (vbuf, vn_s)):
                a = jnp.broadcast_to(new[0, pl.ds(tok, 1), :], (16, 128))
                b = jnp.broadcast_to(new[1, pl.ds(tok, 1), :], (16, 128))
                buf[at, :] = jnp.where(here, jnp.where(odd16, b, a), buf[at, :].astype(F32)).astype(BF16)
        pltpu.make_async_copy(kbuf.at[sl], kout_hbm.at[sl], ko_sem.at[c]).start()
        pltpu.make_async_copy(vbuf.at[sl], vout_hbm.at[sl], vo_sem.at[c]).start()
        for s in range(CHUNK // 8):
            blk = c * (CHUNK // 8) + s
            bs = pl.ds(pl.multiple_of(blk * 512, 512), 512)
            ts = pl.ds(pl.multiple_of(blk * 8, 8), 8)
            q = q_s[blk].reshape(32, 128).astype(BF16)
            sc = lax.dot_general(q, kbuf[bs, :], (((1,), (1,)), ((), ())), preferred_element_type=F32)
            pos = jnp.concatenate([posb_s[ts, :]] * 4, axis=1)
            vis = slot <= pos
            mask = jnp.concatenate([vis & same0] * 2 + [vis & same1] * 2, axis=0)
            sc = jnp.where(mask, sc * 128 ** -0.5, -1e30)
            ex = jnp.exp(sc - jnp.max(sc, axis=1, keepdims=True))
            w = (ex * (1.0 / jnp.sum(ex, axis=1, keepdims=True))).astype(BF16)
            o = jnp.dot(w, vbuf[bs, :], preferred_element_type=F32)
            for k in range(2):
                for n in range(2):
                    o_ref[k, ts, n * 128:(n + 1) * 128] = o[(2 * n + k) * 8:(2 * n + k + 1) * 8]

    @pl.loop(0, chunks)
    def _(c):
        sl = pl.ds(pl.multiple_of(c * crow, crow), crow)
        pltpu.make_async_copy(kbuf.at[sl], kout_hbm.at[sl], ko_sem.at[c]).wait()
        pltpu.make_async_copy(vbuf.at[sl], vout_hbm.at[sl], vo_sem.at[c]).wait()


def attention(pos, meta, x, norm, wkv, router, cos, sin, wq, kc, vc):
    tokens, width = x.shape
    experts, _, qw = wq.shape
    vmem = pl.BlockSpec(memory_space=pltpu.VMEM)
    hbm = pl.BlockSpec(memory_space=pl.ANY)
    chunks = tokens // CHUNK
    return pl.pallas_call(
        qa_kernel,
        name="qkv_attention",
        out_shape=(jax.ShapeDtypeStruct((2, tokens, qw), F32), jax.ShapeDtypeStruct((tokens, 128), F32),
                   jax.ShapeDtypeStruct(kc.shape, BF16), jax.ShapeDtypeStruct(vc.shape, BF16)),
        in_specs=[pl.BlockSpec(memory_space=pltpu.SMEM)] + [vmem] * 7 + [hbm] * 3,
        out_specs=(vmem, vmem, hbm, hbm),
        scratch_shapes=[
            pltpu.VMEM((tokens, width), BF16), pltpu.VMEM(wq.shape, BF16),
            pltpu.VMEM(kc.shape, BF16), pltpu.VMEM(vc.shape, BF16),
            pltpu.VMEM((2, tokens, 128), F32), pltpu.VMEM((2, tokens, 128), F32),
            pltpu.VMEM((tokens // 8, 4, 8, 128), F32), pltpu.VMEM((2, tokens, 128), jnp.int32),
            pltpu.VMEM((tokens, 128), jnp.int32),
            pltpu.SemaphoreType.DMA((experts,))] + [pltpu.SemaphoreType.DMA((chunks,))] * 4,
        compiler_params=pltpu.CompilerParams(vmem_limit_bytes=60 * 2**20),
    )(pos, meta, x, norm, wkv, router, cos, sin, wq, kc, vc)


D2D, RS1, RS2, AGX, AGY, AGS, FWD, FXS, FYS, FDS = range(10)
COLS = 256
FB = 512
SLOTS = 4


def om_kernel(o_ref, ids_ref, gates_ref, x_hbm, norm_ref, router_ref, wo_hbm, wg_hbm, wu_hbm, wd_hbm,
              out_ref,
              wo_s, wg_s, wu_s, wd_s, a_s, u_s, xo_s, xm_s, wb_s, p_s, d_s, s1_s, r1_s, own_s, s2_s, r2_s,
              ssem, rsem, wo_sem, g_sem, up_sem, wd_sem, x_sem):
    tokens, width = u_s.shape
    experts = wo_hbm.shape[0]
    ffn = wg_hbm.shape[1]
    rows = tokens // 8
    blocks = width // COLS
    fblocks = ffn // FB
    dblocks = blocks // 2
    dp, me = lax.axis_index("dp"), lax.axis_index("tp")
    c, xx, yy = me % 2, (me // 2) % 2, me // 4
    sib, xn, yn = me + 1 - 2 * c, me + 2 - 4 * xx, me + 4 - 8 * yy
    dn = xn + 4 - 8 * yy

    def wo_copy(b):
        return pltpu.make_async_copy(wo_hbm.at[:, :, pl.ds(b * COLS, COLS)], wo_s.at[b], wo_sem.at[b])

    def up_copies(f, slot):
        cs = pl.ds(f * FB, FB) if isinstance(f, int) else pl.ds(pl.multiple_of(f * FB, FB), FB)
        return (pltpu.make_async_copy(wg_hbm.at[:, cs], wg_s.at[slot], g_sem.at[slot]),
                pltpu.make_async_copy(wu_hbm.at[:, cs], wu_s.at[slot], up_sem.at[slot]))

    def wd_copy(d):
        return pltpu.make_async_copy(wd_hbm.at[:, pl.ds(d * 2 * COLS, 2 * COLS)], wd_s.at[d % 2], wd_sem.at[d % 2])

    mine = pl.ds(pl.multiple_of(me * rows, rows), rows)
    x_copy = pltpu.make_async_copy(x_hbm.at[mine], xo_s, x_sem)
    for b in range(blocks):
        wo_copy(b).start()
    x_copy.start()
    for f in range(SLOTS):
        for cp in up_copies(f, f):
            cp.start()
    for d in range(2):
        wd_copy(d).start()

    barrier = pltpu.get_barrier_semaphore()
    for other in (sib, xn, yn):
        pl.semaphore_signal(barrier, inc=1, device_id=(dp, other), device_id_type=MESH)

    id0 = jnp.broadcast_to(ids_ref[:, 0:1], (tokens, 128))
    id1 = jnp.broadcast_to(ids_ref[:, 1:2], (tokens, 128))
    for e in range(experts):
        for n in range(2):
            cs = slice(n * 128, (n + 1) * 128)
            a_s[:, e * COLS + n * 128:e * COLS + (n + 1) * 128] = jnp.where(
                id0 == e, o_ref[0, :, cs], jnp.where(id1 == e, o_ref[1, :, cs], 0.0)).astype(BF16)
    x_copy.wait()
    pl.semaphore_wait(barrier, 3)

    def all_reduce(r, produce, lead, dest, finish):
        def remote(stage, b, src, dst, to):
            return pltpu.make_async_remote_copy(src_ref=src, dst_ref=dst, send_sem=ssem.at[r, stage, b], recv_sem=rsem.at[r, stage, b],
                                                device_id=(dp, to), device_id_type=MESH)

        def at(dev, b):
            return dest.at[pl.ds(pl.multiple_of(dev * rows, rows), rows), pl.ds(b * COLS, COLS)]

        def push(stage, b, dev, to):
            return remote(stage, b, at(dev, b), at(dev, b), to)

        def d2d(b):
            return remote(D2D, b, p_s.at[b, :, :, 1 - c], d_s.at[b], sib)

        def rs1(b):
            src = s1_s.at[b, :, 1 - xx] if b % 2 == 0 else s1_s.at[b, 1 - yy]
            return remote(RS1, b, src, r1_s.at[b], xn if b % 2 == 0 else yn)

        def rs2(b):
            return remote(RS2, b, s2_s.at[b], r2_s.at[b], yn if b % 2 == 0 else xn)

        def agx(b):
            return push(AGX, b, me, xn)

        def agy(b):
            return push(AGY, b, me, yn)

        def ags(b):
            return push(AGS, b, me, sib)

        def fwd(b):
            return push(FWD, b, xn, yn) if b % 2 == 0 else push(FWD, b, yn, xn)

        def fxs(b):
            return push(FXS, b, xn, sib)

        def fys(b):
            return push(FYS, b, yn, sib)

        def fds(b):
            return push(FDS, b, dn, sib)

        def st0(b):
            produce(b)
            d2d(b).start()

        def st1(b):
            d2d(b).wait_recv()
            for j in range(2):
                for i in range(2):
                    s1_s[b, j, i] = (p_s[b, j, i, c].astype(F32) + d_s[b, j, i].astype(F32)).astype(BF16)
            rs1(b).start()

        def st2(b):
            rs1(b).wait_recv()
            if b % 2 == 0:
                keep = s1_s[b, yy, xx].astype(F32) + r1_s[b, yy].astype(F32)
                give = s1_s[b, 1 - yy, xx].astype(F32) + r1_s[b, 1 - yy].astype(F32)
            else:
                keep = s1_s[b, yy, xx].astype(F32) + r1_s[b, xx].astype(F32)
                give = s1_s[b, yy, 1 - xx].astype(F32) + r1_s[b, 1 - xx].astype(F32)
            s2_s[b] = give.astype(BF16)
            rs2(b).start()
            own_s[b] = keep

        def st3(b):
            rs2(b).wait_recv()
            finish(b, own_s[b] + r2_s[b].astype(F32))
            for make in (agx, agy, ags):
                make(b).start()

        def st4(b):
            agx(b).wait_recv()
            agy(b).wait_recv()
            for make in (fwd, fxs, fys):
                make(b).start()

        def st5(b):
            fwd(b).wait_recv()
            fds(b).start()

        def st6(b):
            for make in (ags, fxs, fys, fds):
                make(b).wait_recv()

        stages = (st0, st1, st2, st3, st4, st5, st6)
        for i in range(blocks + lead[-1]):
            for stage, lag in zip(stages, lead):
                if 0 <= i - lag < blocks:
                    stage(i - lag)
        for b in range(blocks):
            for make in (d2d, rs1, rs2, agx, agy, ags, fwd, fxs, fys, fds):
                make(b).wait_send()

    def put(b, value):
        p_s[b] = value.astype(BF16).reshape(2, 2, 2, rows, COLS)

    def att_block(b):
        wo_copy(b).wait()
        total = None
        for e in range(experts):
            part = jnp.dot(a_s[:, e * COLS:(e + 1) * COLS], wo_s[b, e], preferred_element_type=F32) * gates_ref[:, e:e + 1]
            total = part if total is None else total + part
        put(b, total)

    def att_finish(b, total):
        cs = slice(b * COLS, (b + 1) * COLS)
        mid = (xo_s[:, cs].astype(F32) + total).astype(BF16)
        xm_s[:, cs] = mid
        u_s[mine, cs] = mid

    all_reduce(0, att_block, (0, 1, 3, 5, 7, 8, 9), u_s, att_finish)
    rms_rows(u_s, norm_ref, u_s, tokens, 32)

    logits = jnp.dot(u_s[...], router_ref[...], preferred_element_type=F32)
    lane = lax.broadcasted_iota(jnp.int32, (tokens, 128), 1)
    id2, id3 = ids_ref[:, 3:4], ids_ref[:, 4:5]
    l0 = jnp.sum(jnp.where(lane == id2, logits, 0.0), axis=1, keepdims=True)
    l1 = jnp.sum(jnp.where(lane == id3, logits, 0.0), axis=1, keepdims=True)
    top = jnp.maximum(l0, l1)
    e0, e1 = jnp.exp(l0 - top), jnp.exp(l1 - top)
    inv = 1.0 / (e0 + e1)
    weight = jnp.where(id2 == me, e0 * inv, 0.0) + jnp.where(id3 == me, e1 * inv, 0.0)
    wb_s[...] = jnp.broadcast_to(weight, (tokens, 128))

    @pl.loop(0, fblocks)
    def _(f):
        slot = f % SLOTS
        for cp in up_copies(f, slot):
            cp.wait()
        g = jnp.dot(u_s[...], wg_s[slot], preferred_element_type=F32)
        up = jnp.dot(u_s[...], wu_s[slot], preferred_element_type=F32)
        a_s[:, pl.ds(pl.multiple_of(f * FB, FB), FB)] = (g * (1.0 / (1.0 + jnp.exp(-g))) * up).astype(BF16)

        @pl.when(f + SLOTS < fblocks)
        def _():
            for cp in up_copies(f + SLOTS, slot):
                cp.start()

    def down_block(b):
        if b % 2:
            return
        d = b // 2
        wd_copy(d).wait()
        y = jnp.dot(a_s[...], wd_s[d % 2], preferred_element_type=F32)
        wb = jnp.concatenate([wb_s[...]] * 2, axis=1)
        for h in range(2):
            put(b + h, y[:, h * COLS:(h + 1) * COLS] * wb)
        if d + 2 < dblocks:
            wd_copy(d + 2).start()

    def down_finish(b, total):
        cs = slice(b * COLS, (b + 1) * COLS)
        out_ref[mine, cs] = (xm_s[:, cs].astype(F32) + total).astype(BF16)

    all_reduce(1, down_block, (0, 2, 3, 5, 7, 8, 9), out_ref, down_finish)


def out_mlp(o, ids, gates, x, norm, router, wo, wg, wu, wd):
    tokens, width = x.shape
    experts = wo.shape[0]
    rows = tokens // 8
    blocks = width // COLS
    vmem = pl.BlockSpec(memory_space=pltpu.VMEM)
    hbm = pl.BlockSpec(memory_space=pl.ANY)
    return pl.pallas_call(
        om_kernel,
        name="out_mlp",
        out_shape=jax.ShapeDtypeStruct((tokens, width), BF16),
        in_specs=[vmem] * 3 + [hbm] + [vmem] * 2 + [hbm] * 4,
        out_specs=vmem,
        scratch_shapes=[
            pltpu.VMEM((blocks, experts, COLS, COLS), BF16),
            pltpu.VMEM((SLOTS, width, FB), BF16), pltpu.VMEM((SLOTS, width, FB), BF16),
            pltpu.VMEM((2, wd.shape[0], 2 * COLS), BF16),
            pltpu.VMEM((tokens, wd.shape[0]), BF16), pltpu.VMEM((tokens, width), BF16),
            pltpu.VMEM((rows, width), BF16), pltpu.VMEM((rows, width), BF16), pltpu.VMEM((tokens, 128), F32),
            pltpu.VMEM((blocks, 2, 2, 2, rows, COLS), BF16), pltpu.VMEM((blocks, 2, 2, rows, COLS), BF16),
            pltpu.VMEM((blocks, 2, 2, rows, COLS), BF16), pltpu.VMEM((blocks, 2, rows, COLS), BF16),
            pltpu.VMEM((blocks, rows, COLS), F32), pltpu.VMEM((blocks, rows, COLS), BF16), pltpu.VMEM((blocks, rows, COLS), BF16),
            pltpu.SemaphoreType.DMA((2, 10, blocks)), pltpu.SemaphoreType.DMA((2, 10, blocks)),
            pltpu.SemaphoreType.DMA((blocks,)), pltpu.SemaphoreType.DMA((SLOTS,)), pltpu.SemaphoreType.DMA((SLOTS,)),
            pltpu.SemaphoreType.DMA((2,)), pltpu.SemaphoreType.DMA],
        compiler_params=pltpu.CompilerParams(vmem_limit_bytes=67043328, collective_id=0, has_side_effects=True),
    )(o, ids, gates, x, norm, router, wo, wg, wu, wd)


def solution(mesh):
    def local_step(x, k_cache, v_cache, positions, att_ids, mlp_ids, norm_att, w_kv, router_att, w_query, w_out, norm_mlp, router_mlp, w_gate, w_up, w_down):
        tokens, width = x.shape
        cache_shape = k_cache.shape
        heads, head_dim = cache_shape[2], cache_shape[3]
        cos, sin = rope_tables(positions, head_dim)
        meta = jnp.concatenate([att_ids, positions[:, None], mlp_ids], axis=1)
        wkv = w_kv.reshape(width, heads, 2, head_dim).transpose(0, 2, 1, 3).reshape(width, 2 * heads * head_dim)
        router = jnp.pad(router_att, ((0, 0), (0, 128 - router_att.shape[1])))
        att, gates, keys_all, values_all = attention(
            positions, meta, x, norm_att[None, :], wkv, router, cos, sin, w_query,
            k_cache.reshape(-1, head_dim), v_cache.reshape(-1, head_dim))
        router2 = jnp.pad(router_mlp, ((0, 0), (0, 128 - router_mlp.shape[1])))
        x_out = out_mlp(att, meta, gates, x, norm_mlp[None, :], router2, w_out, w_gate[0], w_up[0], w_down[0])
        return x_out, keys_all.reshape(cache_shape), values_all.reshape(cache_shape)

    token_spec = P('dp', None)
    cache_spec = P('dp', None, 'tp', None)
    expert_spec = P('tp', None, None)
    in_specs = (token_spec, cache_spec, cache_spec, P('dp'), token_spec, token_spec, P(), P(None, 'tp', None), P(), P(None, None, 'tp'), P(None, 'tp', None), P(), P(), expert_spec, expert_spec, expert_spec)
    out_specs = (token_spec, cache_spec, cache_spec)
    return jax.shard_map(local_step, mesh=mesh, in_specs=in_specs, out_specs=out_specs, check_vma=False)
```

```python
import functools

import jax
import jax.numpy as jnp
from jax import lax
from jax.experimental import pallas as pl
from jax.experimental.pallas import tpu as pltpu
from jax.sharding import PartitionSpec as P

NORM_EPS = 1e-6
ROPE_BASE = 10000.0
F32 = jnp.float32
BF16 = jnp.bfloat16
MESH = pl.DeviceIdType.MESH
CHUNK = 32
SUBS = 4


def rms_rows(x_ref, norm_ref, out_ref, rows, step):
    @pl.loop(0, rows // step)
    def _(i):
        sl = pl.ds(pl.multiple_of(i * step, step), step)
        v = x_ref[sl, :].astype(F32)
        inv = lax.rsqrt(jnp.mean(v * v, axis=-1, keepdims=True) + NORM_EPS)
        out_ref[sl, :] = (v * inv * norm_ref[...]).astype(BF16)


def spread(row):
    return jnp.broadcast_to(row.astype(F32), (128, row.shape[1])).T


def qa_kernel(pos_s, ids_ref, posr_ref, freq_ref, x_ref, norm_ref, wkv_ref, router_ref, wq_hbm, k_hbm, v_hbm,
              o_ref, gates_ref, kout_hbm, vout_hbm,
              h_s, wq_s, wkv_s, kbuf, vbuf, kn_s, vn_s, q_s, idb_s, posb_s, cos_s, sin_s, wq_sem, k_sem, v_sem, ko_sem, vo_sem):
    tokens = x_ref.shape[0]
    experts = wq_hbm.shape[0]
    chunks = tokens // CHUNK
    crow = CHUNK * 64
    per = chunks // experts

    def copies(c):
        sl = pl.ds(c * crow, crow) if isinstance(c, int) else pl.ds(pl.multiple_of(c * crow, crow), crow)
        return (pltpu.make_async_copy(k_hbm.at[sl], kbuf.at[sl], k_sem.at[c]),
                pltpu.make_async_copy(v_hbm.at[sl], vbuf.at[sl], v_sem.at[c]))

    def out_copies(c):
        sl = pl.ds(pl.multiple_of(c * crow, crow), crow)
        return (pltpu.make_async_copy(kbuf.at[sl], kout_hbm.at[sl], ko_sem.at[c]),
                pltpu.make_async_copy(vbuf.at[sl], vout_hbm.at[sl], vo_sem.at[c]))

    def wq_copy(e):
        return pltpu.make_async_copy(wq_hbm.at[e], wq_s.at[e], wq_sem.at[e])

    for e in range(experts):
        wq_copy(e).start()
        for i in range(per):
            for cp in copies(e * per + i):
                cp.start()

    rms_rows(x_ref, norm_ref, h_s, tokens, 32)
    r = lax.broadcasted_iota(jnp.int32, (256, 256), 0)
    swap = (lax.broadcasted_iota(jnp.int32, (256, 256), 1) == 4 * (r % 64) + r // 64).astype(F32).astype(BF16)

    @pl.loop(0, wkv_ref.shape[0] // 1024)
    def _(i):
        for j in range(4):
            part = jnp.dot(swap, wkv_ref[pl.ds(pl.multiple_of(i * 1024 + j * 256, 256), 256), :], preferred_element_type=F32).astype(BF16)
            for n in range(4):
                wkv_s[pl.ds(pl.multiple_of(i * 256 + j * 64, 64), 64), n * 128:(n + 1) * 128] = part[n * 64:(n + 1) * 64]

    for k in range(2):
        idb_s[k] = spread(ids_ref[k:k + 1, :])
    pos = spread(posr_ref[...])
    posb_s[...] = pos.astype(jnp.int32)
    angle = pos * freq_ref[...]
    cos_s[...] = jnp.cos(angle)
    sin = jnp.sin(angle)
    sin_s[...] = jnp.where(lax.broadcasted_iota(jnp.int32, (tokens, 128), 1) < 64, -sin, sin)

    kv = jnp.dot(h_s[...], wkv_s[...], preferred_element_type=F32)
    for n in range(2):
        v = kv[:, n * 128:(n + 1) * 128]
        kn_s[n] = v * cos_s[...] + pltpu.roll(v, 64, 1) * sin_s[...]
        vn_s[n] = kv[:, 256 + n * 128:256 + (n + 1) * 128]
    logits = lax.dot_general(h_s[...], router_ref[...], (((1,), (1,)), ((), ())), preferred_element_type=F32)
    lane = lax.broadcasted_iota(jnp.int32, logits.shape, 1).astype(F32)
    hit0, hit1 = lane == idb_s[0, :, 0:experts], lane == idb_s[1, :, 0:experts]
    l0 = jnp.sum(jnp.where(hit0, logits, 0.0), axis=1, keepdims=True)
    l1 = jnp.sum(jnp.where(hit1, logits, 0.0), axis=1, keepdims=True)
    top = jnp.maximum(l0, l1)
    e0, e1 = jnp.exp(l0 - top), jnp.exp(l1 - top)
    inv = 1.0 / (e0 + e1)
    gates_ref[...] = jnp.where(hit0, e0 * inv, 0.0) + jnp.where(hit1, e1 * inv, 0.0)

    r16 = lax.broadcasted_iota(jnp.int32, (16, 128), 0)
    odd16, pair16 = r16 % 2 == 1, r16 // 2

    @pl.loop(0, experts)
    def _(e):
        wq_copy(e).wait()
        for i in range(per):
            for cp in copies(e * per + i):
                cp.wait()
        q = jnp.dot(h_s[...], wq_s[e], preferred_element_type=F32)
        for t in range(per * CHUNK):
            tok = e * (per * CHUNK) + t
            p = pos_s[tok]
            at = pl.ds(pl.multiple_of(tok * 64 + (p // 8) * 16, 16), 16)
            here = pair16 == p % 8
            for buf, new in ((kbuf, kn_s), (vbuf, vn_s)):
                a = jnp.broadcast_to(new[0, pl.ds(tok, 1), :], (16, 128))
                b = jnp.broadcast_to(new[1, pl.ds(tok, 1), :], (16, 128))
                buf[at, :] = jnp.where(here, jnp.where(odd16, b, a), buf[at, :].astype(F32)).astype(BF16)
        for i in range(per):
            for cp in out_copies(e * per + i):
                cp.start()
        for k in range(2):
            h3 = (idb_s[k] == e.astype(F32)).reshape(tokens // 8, 8, 128)
            for n in range(2):
                part = q[:, n * 128:(n + 1) * 128].reshape(tokens // 8, 8, 128)
                q_s[:, 2 * n + k] = jnp.where(h3, part, q_s[:, 2 * n + k])

    cos3, sin3 = cos_s[...].reshape(tokens // 8, 8, 128), sin_s[...].reshape(tokens // 8, 8, 128)
    for j in range(4):
        v = q_s[:, j]
        q_s[:, j] = v * cos3 + pltpu.roll(v, 64, 2) * sin3

    col = lax.broadcasted_iota(jnp.int32, (8, 512), 1)
    row = lax.broadcasted_iota(jnp.int32, (8, 512), 0)
    slots = [jnp.where((col // 64 == row) & (col % 2 == n), (col % 64) // 2, 1 << 20) for n in range(2)]

    @pl.loop(0, tokens // (8 * SUBS))
    def _(g):
        base = g * SUBS
        rows = [pl.ds(pl.multiple_of((base + s) * 512, 512), 512) for s in range(SUBS)]
        toks = [pl.ds(pl.multiple_of((base + s) * 8, 8), 8) for s in range(SUBS)]
        scores = [lax.dot_general(q_s[base + s].reshape(32, 128).astype(BF16), kbuf[rows[s], :], (((1,), (1,)), ((), ())),
                                  preferred_element_type=F32) for s in range(SUBS)]
        weights = []
        for s in range(SUBS):
            here = jnp.concatenate([posb_s[toks[s], :]] * 4, axis=1)
            vis = [sl <= here for sl in slots]
            mask = jnp.concatenate([vis[0], vis[0], vis[1], vis[1]], axis=0)
            sc = jnp.where(mask, scores[s] * 128 ** -0.5, -1e30)
            ex = jnp.exp(sc - jnp.max(sc, axis=1, keepdims=True))
            weights.append((ex * (1.0 / jnp.sum(ex, axis=1, keepdims=True))).astype(BF16))
        outs = [jnp.dot(weights[s], vbuf[rows[s], :], preferred_element_type=F32) for s in range(SUBS)]
        for s in range(SUBS):
            for k in range(2):
                for n in range(2):
                    o_ref[k, toks[s], n * 128:(n + 1) * 128] = outs[s][(2 * n + k) * 8:(2 * n + k + 1) * 8]

    @pl.loop(0, chunks)
    def _(c):
        for cp in out_copies(c):
            cp.wait()


def attention(pos, ids, posr, freq, x, norm, wkv, router, wq, kc, vc):
    tokens, width = x.shape
    experts, _, qw = wq.shape
    vmem = pl.BlockSpec(memory_space=pltpu.VMEM)
    hbm = pl.BlockSpec(memory_space=pl.ANY)
    chunks = tokens // CHUNK
    return pl.pallas_call(
        qa_kernel,
        name="qkv_attention",
        out_shape=(jax.ShapeDtypeStruct((2, tokens, qw), F32), jax.ShapeDtypeStruct((tokens, experts), F32),
                   jax.ShapeDtypeStruct(kc.shape, BF16), jax.ShapeDtypeStruct(vc.shape, BF16)),
        in_specs=[pl.BlockSpec(memory_space=pltpu.SMEM)] + [vmem] * 7 + [hbm] * 3,
        out_specs=(vmem, vmem, hbm, hbm),
        scratch_shapes=[
            pltpu.VMEM((tokens, width), BF16), pltpu.VMEM(wq.shape, BF16), pltpu.VMEM((width, 512), BF16),
            pltpu.VMEM(kc.shape, BF16), pltpu.VMEM(vc.shape, BF16),
            pltpu.VMEM((2, tokens, 128), F32), pltpu.VMEM((2, tokens, 128), F32),
            pltpu.VMEM((tokens // 8, 4, 8, 128), F32), pltpu.VMEM((2, tokens, 128), F32),
            pltpu.VMEM((tokens, 128), jnp.int32), pltpu.VMEM((tokens, 128), F32), pltpu.VMEM((tokens, 128), F32),
            pltpu.SemaphoreType.DMA((experts,))] + [pltpu.SemaphoreType.DMA((chunks,))] * 4,
        compiler_params=pltpu.CompilerParams(vmem_limit_bytes=60 * 2**20),
    )(pos, ids, posr, freq, x, norm, wkv, router, wq, kc, vc)


D2D, RS1, RS2, AGX, AGY, AGS, FWD, FXS, FYS, FDS = range(10)
COLS = 256
FB = 512
SLOTS = 4
DSLOTS = 4


def om_kernel(o_ref, ids_ref, mids_ref, gates_ref, x_hbm, norm_ref, router_ref, wo_hbm, wg_hbm, wu_hbm, wd_hbm,
              out_ref,
              wo_s, wg_s, wu_s, wd_s, a_s, u_s, xo_s, xm_s, wb_s, p_s, d_s, s1_s, r1_s, own_s, s2_s, r2_s,
              ssem, rsem, wo_sem, g_sem, up_sem, wd_sem, x_sem):
    tokens, width = u_s.shape
    experts = wo_hbm.shape[0]
    ffn = wg_hbm.shape[1]
    rows = tokens // 8
    blocks = width // COLS
    fblocks = ffn // FB
    dp, me = lax.axis_index("dp"), lax.axis_index("tp")
    c, xx, yy = me % 2, (me // 2) % 2, me // 4
    sib, xn, yn = me + 1 - 2 * c, me + 2 - 4 * xx, me + 4 - 8 * yy
    dn = xn + 4 - 8 * yy

    def wo_copy(b):
        return pltpu.make_async_copy(wo_hbm.at[:, :, pl.ds(b * COLS, COLS)], wo_s.at[b], wo_sem.at[b])

    def up_copies(f, slot):
        cs = pl.ds(f * FB, FB) if isinstance(f, int) else pl.ds(pl.multiple_of(f * FB, FB), FB)
        return (pltpu.make_async_copy(wg_hbm.at[:, cs], wg_s.at[slot], g_sem.at[slot]),
                pltpu.make_async_copy(wu_hbm.at[:, cs], wu_s.at[slot], up_sem.at[slot]))

    def wd_copy(d):
        return pltpu.make_async_copy(wd_hbm.at[:, pl.ds(d * COLS, COLS)], wd_s.at[d % DSLOTS], wd_sem.at[d % DSLOTS])

    mine = pl.ds(pl.multiple_of(me * rows, rows), rows)
    x_copy = pltpu.make_async_copy(x_hbm.at[mine], xo_s, x_sem)
    for b in range(blocks):
        wo_copy(b).start()
    x_copy.start()
    for f in range(SLOTS):
        for cp in up_copies(f, f):
            cp.start()
    for d in range(DSLOTS):
        wd_copy(d).start()

    barrier = pltpu.get_barrier_semaphore()
    for other in (sib, xn, yn):
        pl.semaphore_signal(barrier, inc=1, device_id=(dp, other), device_id_type=MESH)

    id0, id1 = spread(ids_ref[0:1, :]), spread(ids_ref[1:2, :])
    for e in range(experts):
        for n in range(2):
            cs = slice(n * 128, (n + 1) * 128)
            a_s[:, e * COLS + n * 128:e * COLS + (n + 1) * 128] = jnp.where(
                id0 == e, o_ref[0, :, cs], jnp.where(id1 == e, o_ref[1, :, cs], 0.0)).astype(BF16)
    x_copy.wait()
    pl.semaphore_wait(barrier, 3)

    def all_reduce(r, produce, lead, dest, finish):
        def remote(stage, b, src, dst, to):
            return pltpu.make_async_remote_copy(src_ref=src, dst_ref=dst, send_sem=ssem.at[r, stage, b], recv_sem=rsem.at[r, stage, b],
                                                device_id=(dp, to), device_id_type=MESH)

        def at(dev, b):
            return dest.at[pl.ds(pl.multiple_of(dev * rows, rows), rows), pl.ds(b * COLS, COLS)]

        def push(stage, b, dev, to):
            return remote(stage, b, at(dev, b), at(dev, b), to)

        def d2d(b):
            return remote(D2D, b, p_s.at[b, :, :, 1 - c], d_s.at[b], sib)

        def rs1(b):
            src = s1_s.at[b, :, 1 - xx] if b % 2 == 0 else s1_s.at[b, 1 - yy]
            return remote(RS1, b, src, r1_s.at[b], xn if b % 2 == 0 else yn)

        def rs2(b):
            return remote(RS2, b, s2_s.at[b], r2_s.at[b], yn if b % 2 == 0 else xn)

        def agx(b):
            return push(AGX, b, me, xn)

        def agy(b):
            return push(AGY, b, me, yn)

        def ags(b):
            return push(AGS, b, me, sib)

        def fwd(b):
            return push(FWD, b, xn, yn) if b % 2 == 0 else push(FWD, b, yn, xn)

        def fxs(b):
            return push(FXS, b, xn, sib)

        def fys(b):
            return push(FYS, b, yn, sib)

        def fds(b):
            return push(FDS, b, dn, sib)

        def st0(b):
            produce(b)
            d2d(b).start()

        def st1(b):
            d2d(b).wait_recv()
            for j in range(2):
                for i in range(2):
                    s1_s[b, j, i] = (p_s[b, j, i, c].astype(F32) + d_s[b, j, i].astype(F32)).astype(BF16)
            rs1(b).start()

        def st2(b):
            rs1(b).wait_recv()
            if b % 2 == 0:
                keep = s1_s[b, yy, xx].astype(F32) + r1_s[b, yy].astype(F32)
                give = s1_s[b, 1 - yy, xx].astype(F32) + r1_s[b, 1 - yy].astype(F32)
            else:
                keep = s1_s[b, yy, xx].astype(F32) + r1_s[b, xx].astype(F32)
                give = s1_s[b, yy, 1 - xx].astype(F32) + r1_s[b, 1 - xx].astype(F32)
            s2_s[b] = give.astype(BF16)
            rs2(b).start()
            own_s[b] = keep

        def st3(b):
            rs2(b).wait_recv()
            finish(b, own_s[b] + r2_s[b].astype(F32))
            for make in (agx, agy, ags):
                make(b).start()

        def st4(b):
            agx(b).wait_recv()
            agy(b).wait_recv()
            for make in (fwd, fxs, fys):
                make(b).start()

        def st5(b):
            fwd(b).wait_recv()
            fds(b).start()

        def st6(b):
            for make in (ags, fxs, fys, fds):
                make(b).wait_recv()

        stages = (st0, st1, st2, st3, st4, st5, st6)
        for i in range(blocks + lead[-1]):
            for stage, lag in zip(stages, lead):
                if 0 <= i - lag < blocks:
                    stage(i - lag)
        for b in range(blocks):
            for make in (d2d, rs1, rs2, agx, agy, ags, fwd, fxs, fys, fds):
                make(b).wait_send()

    def put(b, value):
        p_s[b] = value.astype(BF16).reshape(2, 2, 2, rows, COLS)

    def att_block(b):
        wo_copy(b).wait()
        total = None
        for e in range(experts):
            part = jnp.dot(a_s[:, e * COLS:(e + 1) * COLS], wo_s[b, e], preferred_element_type=F32) * gates_ref[:, e:e + 1]
            total = part if total is None else total + part
        put(b, total)

    def att_finish(b, total):
        cs = slice(b * COLS, (b + 1) * COLS)
        mid = (xo_s[:, cs].astype(F32) + total).astype(BF16)
        xm_s[:, cs] = mid
        u_s[mine, cs] = mid

    all_reduce(0, att_block, (0, 1, 8, 11, 14, 16, 18), u_s, att_finish)
    rms_rows(u_s, norm_ref, u_s, tokens, 32)

    logits = lax.dot_general(u_s[...], router_ref[...], (((1,), (1,)), ((), ())), preferred_element_type=F32)
    lane = lax.broadcasted_iota(jnp.int32, logits.shape, 1).astype(F32)
    id2, id3 = spread(mids_ref[0:1, :]), spread(mids_ref[1:2, :])
    l0 = jnp.sum(jnp.where(lane == id2[:, 0:experts], logits, 0.0), axis=1, keepdims=True)
    l1 = jnp.sum(jnp.where(lane == id3[:, 0:experts], logits, 0.0), axis=1, keepdims=True)
    top = jnp.maximum(l0, l1)
    e0, e1 = jnp.exp(l0 - top), jnp.exp(l1 - top)
    inv = 1.0 / (e0 + e1)
    here = me.astype(F32)
    wb_s[...] = jnp.where(id2 == here, e0 * inv, 0.0) + jnp.where(id3 == here, e1 * inv, 0.0)

    @pl.loop(0, fblocks)
    def _(f):
        slot = f % SLOTS
        for cp in up_copies(f, slot):
            cp.wait()
        g = jnp.dot(u_s[...], wg_s[slot], preferred_element_type=F32)
        up = jnp.dot(u_s[...], wu_s[slot], preferred_element_type=F32)
        a_s[:, pl.ds(pl.multiple_of(f * FB, FB), FB)] = (g * (1.0 / (1.0 + jnp.exp(-g))) * up).astype(BF16)

        @pl.when(f + SLOTS < fblocks)
        def _():
            for cp in up_copies(f + SLOTS, slot):
                cp.start()

    def down_block(b):
        wd_copy(b).wait()
        y = jnp.dot(a_s[...], wd_s[b % DSLOTS], preferred_element_type=F32)
        put(b, y * jnp.concatenate([wb_s[...]] * 2, axis=1))
        if b + DSLOTS < blocks:
            wd_copy(b + DSLOTS).start()

    def down_finish(b, total):
        cs = slice(b * COLS, (b + 1) * COLS)
        out_ref[mine, cs] = (xm_s[:, cs].astype(F32) + total).astype(BF16)

    all_reduce(1, down_block, (0, 1, 4, 7, 10, 12, 14), out_ref, down_finish)


def out_mlp(o, ids, mids, gates, x, norm, router, wo, wg, wu, wd):
    tokens, width = x.shape
    experts = wo.shape[0]
    rows = tokens // 8
    blocks = width // COLS
    vmem = pl.BlockSpec(memory_space=pltpu.VMEM)
    hbm = pl.BlockSpec(memory_space=pl.ANY)
    return pl.pallas_call(
        om_kernel,
        name="out_mlp",
        out_shape=jax.ShapeDtypeStruct((tokens, width), BF16),
        in_specs=[vmem] * 4 + [hbm] + [vmem] * 2 + [hbm] * 4,
        out_specs=vmem,
        scratch_shapes=[
            pltpu.VMEM((blocks, experts, COLS, COLS), BF16),
            pltpu.VMEM((SLOTS, width, FB), BF16), pltpu.VMEM((SLOTS, width, FB), BF16),
            pltpu.VMEM((DSLOTS, wd.shape[0], COLS), BF16),
            pltpu.VMEM((tokens, wd.shape[0]), BF16), pltpu.VMEM((tokens, width), BF16),
            pltpu.VMEM((rows, width), BF16), pltpu.VMEM((rows, width), BF16), pltpu.VMEM((tokens, 128), F32),
            pltpu.VMEM((blocks, 2, 2, 2, rows, COLS), BF16), pltpu.VMEM((blocks, 2, 2, rows, COLS), BF16),
            pltpu.VMEM((blocks, 2, 2, rows, COLS), BF16), pltpu.VMEM((blocks, 2, rows, COLS), BF16),
            pltpu.VMEM((blocks, rows, COLS), F32), pltpu.VMEM((blocks, rows, COLS), BF16), pltpu.VMEM((blocks, rows, COLS), BF16),
            pltpu.SemaphoreType.DMA((2, 10, blocks)), pltpu.SemaphoreType.DMA((2, 10, blocks)),
            pltpu.SemaphoreType.DMA((blocks,)), pltpu.SemaphoreType.DMA((SLOTS,)), pltpu.SemaphoreType.DMA((SLOTS,)),
            pltpu.SemaphoreType.DMA((DSLOTS,)), pltpu.SemaphoreType.DMA],
        compiler_params=pltpu.CompilerParams(vmem_limit_bytes=67043328, collective_id=0, has_side_effects=True),
    )(o, ids, mids, gates, x, norm, router, wo, wg, wu, wd)


def solution(mesh):
    def local_step(x, k_cache, v_cache, positions, att_ids, mlp_ids, norm_att, w_kv, router_att, w_query, w_out, norm_mlp, router_mlp, w_gate, w_up, w_down):
        tokens, width = x.shape
        cache_shape = k_cache.shape
        heads, head_dim = cache_shape[2], cache_shape[3]
        half = jnp.arange(head_dim // 2, dtype=F32)
        freq = ROPE_BASE ** (-(half * 2.0 / head_dim))
        freq = jnp.concatenate([freq, freq])[None, :]
        wkv = w_kv.reshape(width, heads, 2, head_dim).transpose(0, 2, 1, 3).reshape(-1, head_dim)
        att, gates, keys_all, values_all = attention(
            positions, att_ids.T, positions[None, :], freq, x, norm_att[None, :], wkv, router_att.T, w_query,
            k_cache.reshape(-1, head_dim), v_cache.reshape(-1, head_dim))
        x_out = out_mlp(att, att_ids.T, mlp_ids.T, gates, x, norm_mlp[None, :], router_mlp.T, w_out, w_gate[0], w_up[0], w_down[0])
        return x_out, keys_all.reshape(cache_shape), values_all.reshape(cache_shape)

    token_spec = P('dp', None)
    cache_spec = P('dp', None, 'tp', None)
    expert_spec = P('tp', None, None)
    in_specs = (token_spec, cache_spec, cache_spec, P('dp'), token_spec, token_spec, P(), P(None, 'tp', None), P(), P(None, None, 'tp'), P(None, 'tp', None), P(), P(), expert_spec, expert_spec, expert_spec)
    out_specs = (token_spec, cache_spec, cache_spec)
    return jax.shard_map(local_step, mesh=mesh, in_specs=in_specs, out_specs=out_specs, check_vma=False)
```

```python
import jax
import jax.numpy as jnp
import numpy as np
from jax import lax
from jax.experimental import pallas as pl
from jax.experimental.pallas import tpu as pltpu
from jax.sharding import PartitionSpec as P

NORM_EPS = 1e-6
ROPE_BASE = 10000.0
F32 = jnp.float32
BF16 = jnp.bfloat16
MESH = pl.DeviceIdType.MESH
CHUNK = 32
SUBS = 8


def rms_group(x_ref, norm_ref, out_ref, sl):
    v = x_ref[sl, :].astype(F32)
    inv = lax.rsqrt(jnp.mean(v * v, axis=-1, keepdims=True) + NORM_EPS)
    out_ref[sl, :] = (v * inv * norm_ref[...]).astype(BF16)


def rms_rows(x_ref, norm_ref, out_ref, rows, step):
    @pl.loop(0, rows // step)
    def _(i):
        rms_group(x_ref, norm_ref, out_ref, pl.ds(pl.multiple_of(i * step, step), step))


def spread(row):
    return jnp.broadcast_to(row.astype(F32), (128, row.shape[1])).T


def qa_kernel(pos_s, ids_ref, posr_ref, freq_ref, norm_ref, router_ref, x_hbm, wkv_hbm, wq_hbm, k_hbm, v_hbm,
              o_ref, gates_ref, kout_hbm, vout_hbm,
              x_ref, wkv_ref, x_sem, wkv_sem, h_s, wq_s, wkv_s, kbuf, vbuf, kn_s, vn_s, q_s, idb_s, posb_s, cos_s, sin_s, wq_sem, k_sem, v_sem, ko_sem, vo_sem):
    tokens = x_ref.shape[0]
    experts = wq_hbm.shape[0]
    chunks = tokens // CHUNK
    crow = CHUNK * 64
    per = chunks // experts

    def copies(c):
        sl = pl.ds(c * crow, crow) if isinstance(c, int) else pl.ds(pl.multiple_of(c * crow, crow), crow)
        return (pltpu.make_async_copy(k_hbm.at[sl], kbuf.at[sl], k_sem.at[c]),
                pltpu.make_async_copy(v_hbm.at[sl], vbuf.at[sl], v_sem.at[c]))

    def out_copies(c):
        sl = pl.ds(pl.multiple_of(c * crow, crow), crow)
        return (pltpu.make_async_copy(kbuf.at[sl], kout_hbm.at[sl], ko_sem.at[c]),
                pltpu.make_async_copy(vbuf.at[sl], vout_hbm.at[sl], vo_sem.at[c]))

    def wq_copy(e):
        return pltpu.make_async_copy(wq_hbm.at[e], wq_s.at[e], wq_sem.at[e])

    x_copy = pltpu.make_async_copy(x_hbm, x_ref, x_sem)
    wkv_copy = pltpu.make_async_copy(wkv_hbm, wkv_ref, wkv_sem)
    x_copy.start()
    wkv_copy.start()
    for e in range(experts):
        wq_copy(e).start()
        for i in range(per):
            for cp in copies(e * per + i):
                cp.start()

    r = lax.broadcasted_iota(jnp.int32, (256, 256), 0)
    swap = (lax.broadcasted_iota(jnp.int32, (256, 256), 1) == 4 * (r % 64) + r // 64).astype(F32).astype(BF16)

    x_copy.wait()
    wkv_copy.wait()
    steps = wkv_ref.shape[0] // 1024
    group = tokens // steps

    @pl.loop(0, steps)
    def _(i):
        for j in range(4):
            part = jnp.dot(swap, wkv_ref[pl.ds(pl.multiple_of(i * 1024 + j * 256, 256), 256), :], preferred_element_type=F32).astype(BF16)
            for n in range(4):
                wkv_s[pl.ds(pl.multiple_of(i * 256 + j * 64, 64), 64), n * 128:(n + 1) * 128] = part[n * 64:(n + 1) * 64]
        rms_group(x_ref, norm_ref, h_s, pl.ds(pl.multiple_of(i * group, group), group))

    for k in range(2):
        idb_s[k] = spread(ids_ref[k:k + 1, :])
    pos = spread(posr_ref[...])
    posb_s[...] = pos.astype(jnp.int32)
    angle = pos * freq_ref[...]
    cos_s[...] = jnp.cos(angle)
    sin = jnp.sin(angle)
    sin_s[...] = jnp.where(lax.broadcasted_iota(jnp.int32, (tokens, 128), 1) < 64, -sin, sin)

    kv = jnp.dot(h_s[...], wkv_s[...], preferred_element_type=F32)
    for n in range(2):
        v = kv[:, n * 128:(n + 1) * 128]
        kn_s[n] = v * cos_s[...] + pltpu.roll(v, 64, 1) * sin_s[...]
        vn_s[n] = kv[:, 256 + n * 128:256 + (n + 1) * 128]
    logits = lax.dot_general(h_s[...], router_ref[...], (((1,), (1,)), ((), ())), preferred_element_type=F32)
    lane = lax.broadcasted_iota(jnp.int32, logits.shape, 1).astype(F32)
    hit0, hit1 = lane == idb_s[0, :, 0:experts], lane == idb_s[1, :, 0:experts]
    l0 = jnp.sum(jnp.where(hit0, logits, 0.0), axis=1, keepdims=True)
    l1 = jnp.sum(jnp.where(hit1, logits, 0.0), axis=1, keepdims=True)
    top = jnp.maximum(l0, l1)
    e0, e1 = jnp.exp(l0 - top), jnp.exp(l1 - top)
    inv = 1.0 / (e0 + e1)
    gates_ref[...] = jnp.where(lane == 0.0, e0 * inv, e1 * inv)

    r16 = lax.broadcasted_iota(jnp.int32, (16, 128), 0)
    odd16, pair16 = r16 % 2 == 1, r16 // 2

    @pl.loop(0, experts)
    def _(e):
        wq_copy(e).wait()
        for i in range(per):
            for cp in copies(e * per + i):
                cp.wait()
        q = jnp.dot(h_s[...], wq_s[e], preferred_element_type=F32)
        for t in range(per * CHUNK):
            tok = e * (per * CHUNK) + t
            p = pos_s[tok]
            at = pl.ds(pl.multiple_of(tok * 64 + (p // 8) * 16, 16), 16)
            here = pair16 == p % 8
            for buf, new in ((kbuf, kn_s), (vbuf, vn_s)):
                a = jnp.broadcast_to(new[0, pl.ds(tok, 1), :], (16, 128))
                b = jnp.broadcast_to(new[1, pl.ds(tok, 1), :], (16, 128))
                buf[at, :] = jnp.where(here, jnp.where(odd16, b, a), buf[at, :].astype(F32)).astype(BF16)
        for i in range(per):
            for cp in out_copies(e * per + i):
                cp.start()
        for k in range(2):
            h3 = (idb_s[k] == e.astype(F32)).reshape(tokens // 8, 8, 128)
            for n in range(2):
                part = q[:, n * 128:(n + 1) * 128].reshape(tokens // 8, 8, 128)
                q_s[:, 2 * n + k] = jnp.where(h3, part, q_s[:, 2 * n + k])

    cos3, sin3 = cos_s[...].reshape(tokens // 8, 8, 128), sin_s[...].reshape(tokens // 8, 8, 128)
    for j in range(4):
        v = q_s[:, j]
        q_s[:, j] = v * cos3 + pltpu.roll(v, 64, 2) * sin3

    col = lax.broadcasted_iota(jnp.int32, (8, 512), 1)
    row = lax.broadcasted_iota(jnp.int32, (8, 512), 0)
    slots = [jnp.where((col // 64 == row) & (col % 2 == n), (col % 64) // 2, 1 << 20) for n in range(2)]

    @pl.loop(0, tokens // (8 * SUBS))
    def _(g):
        base = g * SUBS
        rows = [pl.ds(pl.multiple_of((base + s) * 512, 512), 512) for s in range(SUBS)]
        toks = [pl.ds(pl.multiple_of((base + s) * 8, 8), 8) for s in range(SUBS)]
        scores = [lax.dot_general(q_s[base + s].reshape(32, 128).astype(BF16), kbuf[rows[s], :], (((1,), (1,)), ((), ())),
                                  preferred_element_type=F32) for s in range(SUBS)]
        weights = []
        for s in range(SUBS):
            here = jnp.concatenate([posb_s[toks[s], :]] * 4, axis=1)
            vis = [sl <= here for sl in slots]
            mask = jnp.concatenate([vis[0], vis[0], vis[1], vis[1]], axis=0)
            sc = jnp.where(mask, scores[s] * 128 ** -0.5, -1e30)
            ex = jnp.exp(sc - jnp.max(sc, axis=1, keepdims=True))
            weights.append((ex * (1.0 / jnp.sum(ex, axis=1, keepdims=True))).astype(BF16))
        outs = [jnp.dot(weights[s], vbuf[rows[s], :], preferred_element_type=F32) for s in range(SUBS)]
        for s in range(SUBS):
            for k in range(2):
                for n in range(2):
                    o_ref[k, toks[s], n * 128:(n + 1) * 128] = outs[s][(2 * n + k) * 8:(2 * n + k + 1) * 8]

    @pl.loop(0, chunks)
    def _(c):
        for cp in out_copies(c):
            cp.wait()


def attention(pos, ids, posr, freq, norm, router, x, wkv, wq, kc, vc):
    tokens, width = x.shape
    experts, _, qw = wq.shape
    vmem = pl.BlockSpec(memory_space=pltpu.VMEM)
    hbm = pl.BlockSpec(memory_space=pl.ANY)
    chunks = tokens // CHUNK
    return pl.pallas_call(
        qa_kernel,
        name="qkv_attention",
        out_shape=(jax.ShapeDtypeStruct((2, tokens, qw), F32), jax.ShapeDtypeStruct((tokens, experts), F32),
                   jax.ShapeDtypeStruct(kc.shape, BF16), jax.ShapeDtypeStruct(vc.shape, BF16)),
        in_specs=[pl.BlockSpec(memory_space=pltpu.SMEM)] + [vmem] * 5 + [hbm] * 5,
        out_specs=(vmem, vmem, hbm, hbm),
        scratch_shapes=[
            pltpu.VMEM(x.shape, BF16), pltpu.VMEM(wkv.shape, BF16), pltpu.SemaphoreType.DMA, pltpu.SemaphoreType.DMA,
            pltpu.VMEM((tokens, width), BF16), pltpu.VMEM(wq.shape, BF16), pltpu.VMEM((width, 512), BF16),
            pltpu.VMEM(kc.shape, BF16), pltpu.VMEM(vc.shape, BF16),
            pltpu.VMEM((2, tokens, 128), F32), pltpu.VMEM((2, tokens, 128), F32),
            pltpu.VMEM((tokens // 8, 4, 8, 128), F32), pltpu.VMEM((2, tokens, 128), F32),
            pltpu.VMEM((tokens, 128), jnp.int32), pltpu.VMEM((tokens, 128), F32), pltpu.VMEM((tokens, 128), F32),
            pltpu.SemaphoreType.DMA((experts,))] + [pltpu.SemaphoreType.DMA((chunks,))] * 4,
        compiler_params=pltpu.CompilerParams(vmem_limit_bytes=60 * 2**20),
    )(pos, ids, posr, freq, norm, router, x, wkv, wq, kc, vc)


D2D, RS1, RS2, AGX, AGY, AGS, FWD, FXS, FYS, FDS = range(10)
COLS = 256
FB = 512
SLOTS = 4
DSLOTS = 4
DIRECT = 2


def om_kernel(o_ref, ids_ref, mids_ref, gates_ref, x_hbm, norm_ref, router_ref, wo_hbm, wg_hbm, wu_hbm, wd_hbm,
              out_ref,
              wo_s, wg_s, wu_s, wd_s, a_s, u_s, xo_s, xm_s, wb_s, g_s, p_s, d_s, s1_s, r1_s, own_s, s2_s, r2_s,
              ssem, rsem, wo_sem, g_sem, up_sem, wd_sem, x_sem):
    tokens, width = u_s.shape
    experts = wo_hbm.shape[0]
    ffn = wg_hbm.shape[1]
    rows = tokens // 8
    blocks = width // COLS
    fblocks = ffn // FB
    dp, me = lax.axis_index("dp"), lax.axis_index("tp")
    c, xx, yy = me % 2, (me // 2) % 2, me // 4
    sib, xn, yn = me + 1 - 2 * c, me + 2 - 4 * xx, me + 4 - 8 * yy
    dn = xn + 4 - 8 * yy

    def cols(b):
        return pl.ds(pl.multiple_of(b * COLS, COLS), COLS)

    def wo_copy(b):
        return pltpu.make_async_copy(wo_hbm.at[:, :, cols(b)], wo_s.at[b], wo_sem.at[b])

    def up_copies(f, slot):
        cs = pl.ds(pl.multiple_of(f * FB, FB), FB)
        return (pltpu.make_async_copy(wg_hbm.at[:, cs], wg_s.at[slot], g_sem.at[slot]),
                pltpu.make_async_copy(wu_hbm.at[:, cs], wu_s.at[slot], up_sem.at[slot]))

    def wd_copy(d):
        return pltpu.make_async_copy(wd_hbm.at[:, cols(d)], wd_s.at[d % DSLOTS], wd_sem.at[d % DSLOTS])

    mine = pl.ds(pl.multiple_of(me * rows, rows), rows)
    x_copy = pltpu.make_async_copy(x_hbm.at[mine], xo_s, x_sem)
    @pl.loop(0, blocks)
    def _(b):
        wo_copy(b).start()

    x_copy.start()

    barrier = pltpu.get_barrier_semaphore()
    for other in (sib, xn, yn, dn):
        pl.semaphore_signal(barrier, inc=1, device_id=(dp, other), device_id_type=MESH)

    id0, id1 = spread(ids_ref[0:1, :]), spread(ids_ref[1:2, :])
    for k, ids in enumerate((id0, id1)):
        for e in range(experts):
            for n in range(2):
                at = (k * experts + e) * COLS + n * 128
                a_s[:, at:at + 128] = jnp.where(ids == e, o_ref[k, :, n * 128:(n + 1) * 128], 0.0).astype(BF16)
        g_s[k] = jnp.broadcast_to(gates_ref[:, k:k + 1], (tokens, 128))
    x_copy.wait()
    pl.semaphore_wait(barrier, 4)

    def all_reduce(r, produce, lead, dest, finish):
        def remote(stage, b, src, dst, to):
            return pltpu.make_async_remote_copy(src_ref=src, dst_ref=dst, send_sem=ssem.at[r, stage, b], recv_sem=rsem.at[r, stage, b],
                                                device_id=(dp, to), device_id_type=MESH)

        def at(dev, b):
            return dest.at[pl.ds(pl.multiple_of(dev * rows, rows), rows), pl.ds(pl.multiple_of(b * COLS, COLS), COLS)]

        def push(stage, b, dev, to):
            return remote(stage, b, at(dev, b), at(dev, b), to)

        def d2d(b, odd):
            return remote(D2D, b, p_s.at[b, :, :, 1 - c], d_s.at[b], sib)

        def rs1(b, odd):
            src = s1_s.at[b, 1 - yy] if odd else s1_s.at[b, :, 1 - xx]
            return remote(RS1, b, src, r1_s.at[b], yn if odd else xn)

        def rs2(b, odd):
            return remote(RS2, b, s2_s.at[b], r2_s.at[b], xn if odd else yn)

        def agx(b, odd):
            return push(AGX, b, me, xn)

        def agy(b, odd):
            return push(AGY, b, me, yn)

        def ags(b, odd):
            return push(AGS, b, me, sib)

        def fwd(b, odd):
            return push(FWD, b, yn, xn) if odd else push(FWD, b, xn, yn)

        def far(b, odd):
            return push(FWD, b, me, dn)

        def fxs(b, odd):
            return push(FXS, b, xn, sib)

        def fys(b, odd):
            return push(FYS, b, yn, sib)

        def fds(b, odd):
            return push(FDS, b, dn, sib)

        def st0(b, odd):
            produce(b)
            d2d(b, odd).start()

        def st1(b, odd):
            d2d(b, odd).wait_recv()
            for j in range(2):
                for i in range(2):
                    s1_s[b, j, i] = (p_s[b, j, i, c].astype(F32) + d_s[b, j, i].astype(F32)).astype(BF16)
            rs1(b, odd).start()

        def st2(b, odd):
            rs1(b, odd).wait_recv()
            keep = s1_s[b, yy, xx].astype(F32)
            if odd:
                keep = keep + r1_s[b, xx].astype(F32)
                give = s1_s[b, yy, 1 - xx].astype(F32) + r1_s[b, 1 - xx].astype(F32)
            else:
                keep = keep + r1_s[b, yy].astype(F32)
                give = s1_s[b, 1 - yy, xx].astype(F32) + r1_s[b, 1 - yy].astype(F32)
            s2_s[b] = give.astype(BF16)
            rs2(b, odd).start()
            own_s[b] = keep

        def st3(b, odd):
            rs2(b, odd).wait_recv()
            finish(b, own_s[b] + r2_s[b].astype(F32))
            agx(b, odd).start()
            agy(b, odd).start()

            @pl.when(b >= blocks - DIRECT)
            def _():
                far(b, odd).start()

            ags(b, odd).start()

        def st4(b, odd):
            agx(b, odd).wait_recv()
            agy(b, odd).wait_recv()

            @pl.when(b < blocks - DIRECT)
            def _():
                fwd(b, odd).start()

            fxs(b, odd).start()
            fys(b, odd).start()

        def st5(b, odd):
            far(b, odd).wait_recv()
            fds(b, odd).start()

        def st6(b, odd):
            for make in (ags, fxs, fys, fds):
                make(b, odd).wait_recv()

        stages = (st0, st1, st2, st3, st4, st5, st6)

        @pl.loop(0, (blocks + lead[-1] + 1) // 2)
        def _(t):
            for half in range(2):
                for stage, lag in zip(stages, lead):
                    b = 2 * t + half - lag

                    @pl.when((b >= 0) & (b < blocks))
                    def _():
                        stage(b, (half - lag) % 2)

        @pl.loop(0, blocks)
        def _(b):
            for make in (d2d, rs1, rs2, agx, agy, ags, far, fxs, fys, fds):
                make(b, 0).wait_send()

    def put(b, value):
        p_s[b] = value.astype(BF16).reshape(2, 2, 2, rows, COLS)

    def att_block(b):
        wo_copy(b).wait()
        w = wo_s[b].reshape(experts * COLS, COLS)
        total = None
        for k in range(2):
            part = jnp.dot(a_s[:, k * experts * COLS:(k + 1) * experts * COLS], w, preferred_element_type=F32)
            part = part * jnp.concatenate([g_s[k]] * 2, axis=1)
            total = part if total is None else total + part
        put(b, total)

        @pl.when(b < SLOTS)
        def _():
            for cp in up_copies(b, b):
                cp.start()

        @pl.when((b >= SLOTS) & (b < SLOTS + DSLOTS))
        def _():
            wd_copy(b - SLOTS).start()

    def att_finish(b, total):
        cs = cols(b)
        mid = (xo_s[:, cs].astype(F32) + total).astype(BF16)
        xm_s[:, cs] = mid
        u_s[mine, cs] = mid

    all_reduce(0, att_block, (0, 1, 4, 7, 10, 12, 14), u_s, att_finish)
    rms_rows(u_s, norm_ref, u_s, tokens, 128)

    logits = lax.dot_general(u_s[...], router_ref[...], (((1,), (1,)), ((), ())), preferred_element_type=F32)
    lane = lax.broadcasted_iota(jnp.int32, logits.shape, 1).astype(F32)
    id2, id3 = spread(mids_ref[0:1, :]), spread(mids_ref[1:2, :])
    l0 = jnp.sum(jnp.where(lane == id2[:, 0:experts], logits, 0.0), axis=1, keepdims=True)
    l1 = jnp.sum(jnp.where(lane == id3[:, 0:experts], logits, 0.0), axis=1, keepdims=True)
    top = jnp.maximum(l0, l1)
    e0, e1 = jnp.exp(l0 - top), jnp.exp(l1 - top)
    inv = 1.0 / (e0 + e1)
    here = me.astype(F32)
    wb_s[...] = jnp.where(id2 == here, e0 * inv, 0.0) + jnp.where(id3 == here, e1 * inv, 0.0)

    @pl.loop(0, fblocks)
    def _(f):
        slot = f % SLOTS
        for cp in up_copies(f, slot):
            cp.wait()
        g = jnp.dot(u_s[...], wg_s[slot], preferred_element_type=F32)
        up = jnp.dot(u_s[...], wu_s[slot], preferred_element_type=F32)
        a_s[:, pl.ds(pl.multiple_of(f * FB, FB), FB)] = (g * (1.0 / (1.0 + jnp.exp(-g))) * up).astype(BF16)

        @pl.when(f + SLOTS < fblocks)
        def _():
            for cp in up_copies(f + SLOTS, slot):
                cp.start()

    def down_block(b):
        wd_copy(b).wait()
        y = jnp.dot(a_s[...], wd_s[b % DSLOTS], preferred_element_type=F32)
        put(b, y * jnp.concatenate([wb_s[...]] * 2, axis=1))

        @pl.when(b + DSLOTS < blocks)
        def _():
            wd_copy(b + DSLOTS).start()

    def down_finish(b, total):
        cs = cols(b)
        out_ref[mine, cs] = (xm_s[:, cs].astype(F32) + total).astype(BF16)

    all_reduce(1, down_block, (0, 1, 3, 5, 7, 9, 11), out_ref, down_finish)


def out_mlp(o, ids, mids, gates, x, norm, router, wo, wg, wu, wd):
    tokens, width = x.shape
    experts = wo.shape[0]
    rows = tokens // 8
    blocks = width // COLS
    vmem = pl.BlockSpec(memory_space=pltpu.VMEM)
    hbm = pl.BlockSpec(memory_space=pl.ANY)
    return pl.pallas_call(
        om_kernel,
        name="out_mlp",
        out_shape=jax.ShapeDtypeStruct((tokens, width), BF16),
        in_specs=[vmem] * 4 + [hbm] + [vmem] * 2 + [hbm] * 4,
        out_specs=vmem,
        scratch_shapes=[
            pltpu.VMEM((blocks, experts, COLS, COLS), BF16),
            pltpu.VMEM((SLOTS, width, FB), BF16), pltpu.VMEM((SLOTS, width, FB), BF16),
            pltpu.VMEM((DSLOTS, wd.shape[0], COLS), BF16),
            pltpu.VMEM((tokens, wd.shape[0]), BF16), pltpu.VMEM((tokens, width), BF16),
            pltpu.VMEM((rows, width), BF16), pltpu.VMEM((rows, width), BF16), pltpu.VMEM((tokens, 128), F32), pltpu.VMEM((2, tokens, 128), F32),
            pltpu.VMEM((blocks, 2, 2, 2, rows, COLS), BF16), pltpu.VMEM((blocks, 2, 2, rows, COLS), BF16),
            pltpu.VMEM((blocks, 2, 2, rows, COLS), BF16), pltpu.VMEM((blocks, 2, rows, COLS), BF16),
            pltpu.VMEM((blocks, rows, COLS), F32), pltpu.VMEM((blocks, rows, COLS), BF16), pltpu.VMEM((blocks, rows, COLS), BF16),
            pltpu.SemaphoreType.DMA((2, 10, blocks)), pltpu.SemaphoreType.DMA((2, 10, blocks)),
            pltpu.SemaphoreType.DMA((blocks,)), pltpu.SemaphoreType.DMA((SLOTS,)), pltpu.SemaphoreType.DMA((SLOTS,)),
            pltpu.SemaphoreType.DMA((DSLOTS,)), pltpu.SemaphoreType.DMA],
        compiler_params=pltpu.CompilerParams(vmem_limit_bytes=67043328, collective_id=0, has_side_effects=True),
    )(o, ids, mids, gates, x, norm, router, wo, wg, wu, wd)


def solution(mesh):
    def local_step(x, k_cache, v_cache, positions, att_ids, mlp_ids, norm_att, w_kv, router_att, w_query, w_out, norm_mlp, router_mlp, w_gate, w_up, w_down):
        tokens, width = x.shape
        cache_shape = k_cache.shape
        heads, head_dim = cache_shape[2], cache_shape[3]
        half = np.arange(head_dim // 2, dtype=np.float64)
        freq = (ROPE_BASE ** (-(half * 2.0 / head_dim))).astype(np.float32)
        freq = np.concatenate([freq, freq])[None, :]
        wkv = w_kv.reshape(width, heads, 2, head_dim).transpose(0, 2, 1, 3).reshape(-1, head_dim)
        att, gates, keys_all, values_all = attention(
            positions, att_ids.T, positions[None, :], freq, norm_att[None, :], router_att.T, x, wkv, w_query,
            k_cache.reshape(-1, head_dim), v_cache.reshape(-1, head_dim))
        x_out = out_mlp(att, att_ids.T, mlp_ids.T, gates, x, norm_mlp[None, :], router_mlp.T, w_out, w_gate[0], w_up[0], w_down[0])
        return x_out, keys_all.reshape(cache_shape), values_all.reshape(cache_shape)

    token_spec = P('dp', None)
    cache_spec = P('dp', None, 'tp', None)
    expert_spec = P('tp', None, None)
    in_specs = (token_spec, cache_spec, cache_spec, P('dp'), token_spec, token_spec, P(), P(None, 'tp', None), P(), P(None, None, 'tp'), P(None, 'tp', None), P(), P(), expert_spec, expert_spec, expert_spec)
    out_specs = (token_spec, cache_spec, cache_spec)
    return jax.shard_map(local_step, mesh=mesh, in_specs=in_specs, out_specs=out_specs, check_vma=False)
```

```python
import jax
import jax.numpy as jnp
import numpy as np
from jax import lax
from jax.experimental import pallas as pl
from jax.experimental.pallas import tpu as pltpu
from jax.sharding import PartitionSpec as P

NORM_EPS = 1e-6
ROPE_BASE = 10000.0
F32 = jnp.float32
BF16 = jnp.bfloat16
MESH = pl.DeviceIdType.MESH
CHUNK = 32
LIM = 60 * 2**20
SUBS = 16


def rms_group(x_ref, norm_ref, out_ref, sl):
    v = x_ref[sl, :].astype(F32)
    inv = lax.rsqrt(jnp.mean(v * v, axis=-1, keepdims=True) + NORM_EPS)
    out_ref[sl, :] = (v * inv * norm_ref[...]).astype(BF16)


def rms_rows(x_ref, norm_ref, out_ref, rows, step):
    @pl.loop(0, rows // step)
    def _(i):
        rms_group(x_ref, norm_ref, out_ref, pl.ds(pl.multiple_of(i * step, step), step))


def spread(row):
    return jnp.broadcast_to(row.astype(F32), (128, row.shape[1])).T


def qa_kernel(pos_s, ids_ref, posr_ref, freq_ref, norm_ref, router_ref, x_hbm, wkv_hbm, wq_hbm, k_hbm, v_hbm,
              o_ref, gates_ref, kout_hbm, vout_hbm,
              x_ref, wkv_ref, x_sem, wkv_sem, h_s, wq_s, wkv_s, kbuf, vbuf, kn_s, vn_s, q_s, idb_s, posb_s, cos_s, sin_s, wq_sem, k_sem, v_sem, ko_sem, vo_sem):
    tokens = x_ref.shape[0]
    experts = wq_hbm.shape[0]
    chunks = tokens // CHUNK
    crow = CHUNK * 64
    per = chunks // experts

    def copies(c):
        sl = pl.ds(pl.multiple_of(c * crow, crow), crow)
        return (pltpu.make_async_copy(k_hbm.at[sl], kbuf.at[sl], k_sem.at[c]),
                pltpu.make_async_copy(v_hbm.at[sl], vbuf.at[sl], v_sem.at[c]))

    def out_copies(c):
        sl = pl.ds(pl.multiple_of(c * crow, crow), crow)
        return (pltpu.make_async_copy(kbuf.at[sl], kout_hbm.at[sl], ko_sem.at[c]),
                pltpu.make_async_copy(vbuf.at[sl], vout_hbm.at[sl], vo_sem.at[c]))

    def wq_copy(e):
        return pltpu.make_async_copy(wq_hbm.at[e], wq_s.at[e], wq_sem.at[e])

    x_copy = pltpu.make_async_copy(x_hbm, x_ref, x_sem)
    wkv_copy = pltpu.make_async_copy(wkv_hbm, wkv_ref, wkv_sem)
    x_copy.start()
    wkv_copy.start()
    r = lax.broadcasted_iota(jnp.int32, (256, 256), 0)
    swap = (lax.broadcasted_iota(jnp.int32, (256, 256), 1) == 4 * (r % 64) + r // 64).astype(F32).astype(BF16)

    x_copy.wait()
    wkv_copy.wait()
    steps = wkv_ref.shape[0] // 1024
    group = tokens // steps

    @pl.loop(0, steps)
    def _(i):
        wq_copy(i).start()
        for j in range(per):
            for cp in copies(i * per + j):
                cp.start()
        for j in range(4):
            part = jnp.dot(swap, wkv_ref[pl.ds(pl.multiple_of(i * 1024 + j * 256, 256), 256), :], preferred_element_type=F32).astype(BF16)
            for n in range(4):
                wkv_s[pl.ds(pl.multiple_of(i * 256 + j * 64, 64), 64), n * 128:(n + 1) * 128] = part[n * 64:(n + 1) * 64]
        rms_group(x_ref, norm_ref, h_s, pl.ds(pl.multiple_of(i * group, group), group))

    for k in range(2):
        idb_s[k] = spread(ids_ref[k:k + 1, :])
    pos = spread(posr_ref[...])
    posb_s[...] = pos.astype(jnp.int32)
    angle = pos * freq_ref[...]
    cos_s[...] = jnp.cos(angle)
    sin = jnp.sin(angle)
    sin_s[...] = jnp.where(lax.broadcasted_iota(jnp.int32, (tokens, 128), 1) < 64, -sin, sin)

    kv = jnp.dot(h_s[...], wkv_s[...], preferred_element_type=F32)
    for n in range(2):
        v = kv[:, n * 128:(n + 1) * 128]
        kn_s[n] = v * cos_s[...] + pltpu.roll(v, 64, 1) * sin_s[...]
        vn_s[n] = kv[:, 256 + n * 128:256 + (n + 1) * 128]
    logits = lax.dot_general(h_s[...], router_ref[...], (((1,), (1,)), ((), ())), preferred_element_type=F32)
    lane = lax.broadcasted_iota(jnp.int32, logits.shape, 1).astype(F32)
    hit0, hit1 = lane == idb_s[0, :, 0:experts], lane == idb_s[1, :, 0:experts]
    l0 = jnp.sum(jnp.where(hit0, logits, 0.0), axis=1, keepdims=True)
    l1 = jnp.sum(jnp.where(hit1, logits, 0.0), axis=1, keepdims=True)
    top = jnp.maximum(l0, l1)
    e0, e1 = jnp.exp(l0 - top), jnp.exp(l1 - top)
    inv = 1.0 / (e0 + e1)
    gates_ref[...] = jnp.where(lane == 0.0, e0 * inv, e1 * inv)

    r16 = lax.broadcasted_iota(jnp.int32, (16, 128), 0)
    odd16, pair16 = r16 % 2 == 1, r16 // 2

    @pl.loop(0, experts)
    def _(e):
        wq_copy(e).wait()
        for i in range(per):
            for cp in copies(e * per + i):
                cp.wait()
        q = jnp.dot(h_s[...], wq_s[e], preferred_element_type=F32)
        for t in range(per * CHUNK):
            tok = e * (per * CHUNK) + t
            p = pos_s[tok]
            at = pl.ds(pl.multiple_of(tok * 64 + (p // 8) * 16, 16), 16)
            here = pair16 == p % 8
            for buf, new in ((kbuf, kn_s), (vbuf, vn_s)):
                a = jnp.broadcast_to(new[0, pl.ds(tok, 1), :], (16, 128))
                b = jnp.broadcast_to(new[1, pl.ds(tok, 1), :], (16, 128))
                buf[at, :] = jnp.where(here, jnp.where(odd16, b, a), buf[at, :].astype(F32)).astype(BF16)
        for i in range(per):
            for cp in out_copies(e * per + i):
                cp.start()
        for k in range(2):
            h3 = (idb_s[k] == e.astype(F32)).reshape(tokens // 8, 8, 128)
            for n in range(2):
                part = q[:, n * 128:(n + 1) * 128].reshape(tokens // 8, 8, 128)
                q_s[:, 2 * n + k] = jnp.where(h3, part, q_s[:, 2 * n + k])

    cos3, sin3 = cos_s[...].reshape(tokens // 8, 8, 128), sin_s[...].reshape(tokens // 8, 8, 128)
    for j in range(4):
        v = q_s[:, j]
        q_s[:, j] = v * cos3 + pltpu.roll(v, 64, 2) * sin3

    col = lax.broadcasted_iota(jnp.int32, (8, 512), 1)
    row = lax.broadcasted_iota(jnp.int32, (8, 512), 0)
    slots = [jnp.where((col // 64 == row) & (col % 2 == n), (col % 64) // 2, 1 << 20) for n in range(2)]

    @pl.loop(0, tokens // (8 * SUBS))
    def _(g):
        base = g * SUBS
        rows = [pl.ds(pl.multiple_of((base + s) * 512, 512), 512) for s in range(SUBS)]
        toks = [pl.ds(pl.multiple_of((base + s) * 8, 8), 8) for s in range(SUBS)]
        scores = [lax.dot_general(q_s[base + s].reshape(32, 128).astype(BF16), kbuf[rows[s], :], (((1,), (1,)), ((), ())),
                                  preferred_element_type=F32) for s in range(SUBS)]
        weights = []
        for s in range(SUBS):
            here = jnp.concatenate([posb_s[toks[s], :]] * 4, axis=1)
            vis = [sl <= here for sl in slots]
            mask = jnp.concatenate([vis[0], vis[0], vis[1], vis[1]], axis=0)
            sc = jnp.where(mask, scores[s] * 128 ** -0.5, -1e30)
            ex = jnp.exp(sc - jnp.max(sc, axis=1, keepdims=True))
            weights.append((ex * (1.0 / jnp.sum(ex, axis=1, keepdims=True))).astype(BF16))
        outs = [jnp.dot(weights[s], vbuf[rows[s], :], preferred_element_type=F32) for s in range(SUBS)]
        for s in range(SUBS):
            for k in range(2):
                for n in range(2):
                    o_ref[k, toks[s], n * 128:(n + 1) * 128] = outs[s][(2 * n + k) * 8:(2 * n + k + 1) * 8]

    @pl.loop(0, chunks)
    def _(c):
        for cp in out_copies(c):
            cp.wait()


def attention(pos, ids, posr, freq, norm, router, x, wkv, wq, kc, vc):
    tokens, width = x.shape
    experts, _, qw = wq.shape
    vmem = pl.BlockSpec(memory_space=pltpu.VMEM)
    hbm = pl.BlockSpec(memory_space=pl.ANY)
    chunks = tokens // CHUNK
    return pl.pallas_call(
        qa_kernel,
        name="qkv_attention",
        out_shape=(jax.ShapeDtypeStruct((2, tokens, qw), F32), jax.ShapeDtypeStruct((tokens, experts), F32),
                   jax.ShapeDtypeStruct(kc.shape, BF16), jax.ShapeDtypeStruct(vc.shape, BF16)),
        in_specs=[pl.BlockSpec(memory_space=pltpu.SMEM)] + [vmem] * 5 + [hbm] * 5,
        out_specs=(vmem, vmem, hbm, hbm),
        scratch_shapes=[
            pltpu.VMEM(x.shape, BF16), pltpu.VMEM(wkv.shape, BF16), pltpu.SemaphoreType.DMA, pltpu.SemaphoreType.DMA,
            pltpu.VMEM((tokens, width), BF16), pltpu.VMEM(wq.shape, BF16), pltpu.VMEM((width, 512), BF16),
            pltpu.VMEM(kc.shape, BF16), pltpu.VMEM(vc.shape, BF16),
            pltpu.VMEM((2, tokens, 128), F32), pltpu.VMEM((2, tokens, 128), F32),
            pltpu.VMEM((tokens // 8, 4, 8, 128), F32), pltpu.VMEM((2, tokens, 128), F32),
            pltpu.VMEM((tokens, 128), jnp.int32), pltpu.VMEM((tokens, 128), F32), pltpu.VMEM((tokens, 128), F32),
            pltpu.SemaphoreType.DMA((experts,))] + [pltpu.SemaphoreType.DMA((chunks,))] * 4,
        compiler_params=pltpu.CompilerParams(vmem_limit_bytes=60 * 2**20),
    )(pos, ids, posr, freq, norm, router, x, wkv, wq, kc, vc)


D2D, RS1, RS2, AGX, AGY, AGS, FWD, FXS, FYS, FDS = range(10)
COLS = 256
FB = 512
SLOTS = 4
DSLOTS = 4
DIRECT = 2


def om_kernel(o_ref, ids_ref, mids_ref, gates_ref, x_hbm, norm_ref, router_ref, wo_hbm, wg_hbm, wu_hbm, wd_hbm,
              out_ref,
              wo_s, wg_s, wu_s, wd_s, a_s, u_s, xo_s, xm_s, wb_s, g_s, p_s, d_s, s1_s, r1_s, own_s, s2_s, r2_s,
              ssem, rsem, wo_sem, g_sem, up_sem, wd_sem, x_sem):
    tokens, width = u_s.shape
    experts = wo_hbm.shape[0]
    ffn = wg_hbm.shape[1]
    rows = tokens // 8
    blocks = width // COLS
    fblocks = ffn // FB
    dp, me = lax.axis_index("dp"), lax.axis_index("tp")
    c, xx, yy = me % 2, (me // 2) % 2, me // 4
    sib, xn, yn = me + 1 - 2 * c, me + 2 - 4 * xx, me + 4 - 8 * yy
    dn = xn + 4 - 8 * yy

    def cols(b):
        return pl.ds(pl.multiple_of(b * COLS, COLS), COLS)

    def wo_copy(b):
        return pltpu.make_async_copy(wo_hbm.at[:, :, cols(b)], wo_s.at[b], wo_sem.at[b])

    def up_copies(f, slot):
        cs = pl.ds(pl.multiple_of(f * FB, FB), FB)
        return (pltpu.make_async_copy(wg_hbm.at[:, cs], wg_s.at[slot], g_sem.at[slot]),
                pltpu.make_async_copy(wu_hbm.at[:, cs], wu_s.at[slot], up_sem.at[slot]))

    def wd_copy(d):
        return pltpu.make_async_copy(wd_hbm.at[:, cols(d)], wd_s.at[d % DSLOTS], wd_sem.at[d % DSLOTS])

    mine = pl.ds(pl.multiple_of(me * rows, rows), rows)
    x_copy = pltpu.make_async_copy(x_hbm.at[mine], xo_s, x_sem)
    @pl.loop(0, blocks)
    def _(b):
        wo_copy(b).start()

    x_copy.start()

    barrier = pltpu.get_barrier_semaphore()
    for other in (sib, xn, yn, dn):
        pl.semaphore_signal(barrier, inc=1, device_id=(dp, other), device_id_type=MESH)

    id0, id1 = spread(ids_ref[0:1, :]), spread(ids_ref[1:2, :])
    for k, ids in enumerate((id0, id1)):
        for e in range(experts):
            for n in range(2):
                at = (k * experts + e) * COLS + n * 128
                a_s[:, at:at + 128] = jnp.where(ids == e, o_ref[k, :, n * 128:(n + 1) * 128], 0.0).astype(BF16)
        g_s[k] = jnp.broadcast_to(gates_ref[:, k:k + 1], (tokens, 128))
    x_copy.wait()
    pl.semaphore_wait(barrier, 4)

    def all_reduce(r, produce, lead, dest, finish):
        def remote(stage, b, src, dst, to):
            return pltpu.make_async_remote_copy(src_ref=src, dst_ref=dst, send_sem=ssem.at[r, stage, b], recv_sem=rsem.at[r, stage, b],
                                                device_id=(dp, to), device_id_type=MESH)

        def at(dev, b):
            return dest.at[pl.ds(pl.multiple_of(dev * rows, rows), rows), pl.ds(pl.multiple_of(b * COLS, COLS), COLS)]

        def push(stage, b, dev, to):
            return remote(stage, b, at(dev, b), at(dev, b), to)

        def d2d(b, odd):
            return remote(D2D, b, p_s.at[b, :, :, 1 - c], d_s.at[b], sib)

        def rs1(b, odd):
            src = s1_s.at[b, 1 - yy] if odd else s1_s.at[b, :, 1 - xx]
            return remote(RS1, b, src, r1_s.at[b], yn if odd else xn)

        def rs2(b, odd):
            return remote(RS2, b, s2_s.at[b], r2_s.at[b], xn if odd else yn)

        def agx(b, odd):
            return push(AGX, b, me, xn)

        def agy(b, odd):
            return push(AGY, b, me, yn)

        def ags(b, odd):
            return push(AGS, b, me, sib)

        def fwd(b, odd):
            return push(FWD, b, yn, xn) if odd else push(FWD, b, xn, yn)

        def far(b, odd):
            return push(FWD, b, me, dn)

        def fxs(b, odd):
            return push(FXS, b, xn, sib)

        def fys(b, odd):
            return push(FYS, b, yn, sib)

        def fds(b, odd):
            return push(FDS, b, dn, sib)

        def st0(b, odd):
            produce(b)
            d2d(b, odd).start()

        def st1(b, odd):
            d2d(b, odd).wait_recv()
            for j in range(2):
                for i in range(2):
                    s1_s[b, j, i] = (p_s[b, j, i, c].astype(F32) + d_s[b, j, i].astype(F32)).astype(BF16)
            rs1(b, odd).start()

        def st2(b, odd):
            rs1(b, odd).wait_recv()
            keep = s1_s[b, yy, xx].astype(F32)
            if odd:
                keep = keep + r1_s[b, xx].astype(F32)
                give = s1_s[b, yy, 1 - xx].astype(F32) + r1_s[b, 1 - xx].astype(F32)
            else:
                keep = keep + r1_s[b, yy].astype(F32)
                give = s1_s[b, 1 - yy, xx].astype(F32) + r1_s[b, 1 - yy].astype(F32)
            s2_s[b] = give.astype(BF16)
            rs2(b, odd).start()
            own_s[b] = keep

        def st3(b, odd):
            rs2(b, odd).wait_recv()
            finish(b, own_s[b] + r2_s[b].astype(F32))
            agx(b, odd).start()
            agy(b, odd).start()

            @pl.when(b >= blocks - DIRECT)
            def _():
                far(b, odd).start()

            ags(b, odd).start()

        def st4(b, odd):
            agx(b, odd).wait_recv()
            agy(b, odd).wait_recv()

            @pl.when(b < blocks - DIRECT)
            def _():
                fwd(b, odd).start()

            fxs(b, odd).start()
            fys(b, odd).start()

        def st5(b, odd):
            far(b, odd).wait_recv()
            fds(b, odd).start()

        def st6(b, odd):
            for make in (ags, fxs, fys, fds):
                make(b, odd).wait_recv()

        stages = (st0, st1, st2, st3, st4, st5, st6)

        @pl.loop(0, (blocks + lead[-1] + 1) // 2)
        def _(t):
            for half in range(2):
                for stage, lag in zip(stages, lead):
                    b = 2 * t + half - lag

                    @pl.when((b >= 0) & (b < blocks))
                    def _():
                        stage(b, (half - lag) % 2)

        @pl.loop(0, blocks)
        def _(b):
            for make in (d2d, rs1, rs2, agx, agy, ags, far, fxs, fys, fds):
                make(b, 0).wait_send()

    def put(b, value):
        p_s[b] = value.astype(BF16).reshape(2, 2, 2, rows, COLS)

    def att_block(b):
        wo_copy(b).wait()
        w = wo_s[b].reshape(experts * COLS, COLS)
        total = None
        for k in range(2):
            part = jnp.dot(a_s[:, k * experts * COLS:(k + 1) * experts * COLS], w, preferred_element_type=F32)
            part = part * jnp.concatenate([g_s[k]] * 2, axis=1)
            total = part if total is None else total + part
        put(b, total)

        @pl.when(b < SLOTS)
        def _():
            for cp in up_copies(b, b):
                cp.start()

        @pl.when((b >= SLOTS) & (b < SLOTS + DSLOTS))
        def _():
            wd_copy(b - SLOTS).start()

    def att_finish(b, total):
        cs = cols(b)
        mid = (xo_s[:, cs].astype(F32) + total).astype(BF16)
        xm_s[:, cs] = mid
        u_s[mine, cs] = mid

    all_reduce(0, att_block, (0, 1, 3, 5, 7, 9, 11), u_s, att_finish)
    rms_rows(u_s, norm_ref, u_s, tokens, 128)

    logits = lax.dot_general(u_s[...], router_ref[...], (((1,), (1,)), ((), ())), preferred_element_type=F32)
    lane = lax.broadcasted_iota(jnp.int32, logits.shape, 1).astype(F32)
    id2, id3 = spread(mids_ref[0:1, :]), spread(mids_ref[1:2, :])
    l0 = jnp.sum(jnp.where(lane == id2[:, 0:experts], logits, 0.0), axis=1, keepdims=True)
    l1 = jnp.sum(jnp.where(lane == id3[:, 0:experts], logits, 0.0), axis=1, keepdims=True)
    top = jnp.maximum(l0, l1)
    e0, e1 = jnp.exp(l0 - top), jnp.exp(l1 - top)
    inv = 1.0 / (e0 + e1)
    here = me.astype(F32)
    wb_s[...] = jnp.where(id2 == here, e0 * inv, 0.0) + jnp.where(id3 == here, e1 * inv, 0.0)

    @pl.loop(0, fblocks)
    def _(f):
        slot = f % SLOTS
        for cp in up_copies(f, slot):
            cp.wait()
        g = jnp.dot(u_s[...], wg_s[slot], preferred_element_type=F32)
        up = jnp.dot(u_s[...], wu_s[slot], preferred_element_type=F32)
        a_s[:, pl.ds(pl.multiple_of(f * FB, FB), FB)] = (g * (1.0 / (1.0 + jnp.exp(-g))) * up).astype(BF16)

        @pl.when(f + SLOTS < fblocks)
        def _():
            for cp in up_copies(f + SLOTS, slot):
                cp.start()

    def down_block(b):
        wd_copy(b).wait()
        y = jnp.dot(a_s[...], wd_s[b % DSLOTS], preferred_element_type=F32)
        put(b, y * jnp.concatenate([wb_s[...]] * 2, axis=1))

        @pl.when(b + DSLOTS < blocks)
        def _():
            wd_copy(b + DSLOTS).start()

    def down_finish(b, total):
        cs = cols(b)
        out_ref[mine, cs] = (xm_s[:, cs].astype(F32) + total).astype(BF16)

    all_reduce(1, down_block, (0, 1, 3, 5, 7, 9, 11), out_ref, down_finish)


def out_mlp(o, ids, mids, gates, x, norm, router, wo, wg, wu, wd):
    tokens, width = x.shape
    experts = wo.shape[0]
    rows = tokens // 8
    blocks = width // COLS
    vmem = pl.BlockSpec(memory_space=pltpu.VMEM)
    hbm = pl.BlockSpec(memory_space=pl.ANY)
    return pl.pallas_call(
        om_kernel,
        name="out_mlp",
        out_shape=pltpu.VMEM((tokens, width), BF16),
        in_specs=[vmem] * 4 + [hbm] + [vmem] * 2 + [hbm] * 4,
        out_specs=vmem,
        scratch_shapes=[
            pltpu.VMEM((blocks, experts, COLS, COLS), BF16),
            pltpu.VMEM((SLOTS, width, FB), BF16), pltpu.VMEM((SLOTS, width, FB), BF16),
            pltpu.VMEM((DSLOTS, wd.shape[0], COLS), BF16),
            pltpu.VMEM((tokens, wd.shape[0]), BF16), pltpu.VMEM((tokens, width), BF16),
            pltpu.VMEM((rows, width), BF16), pltpu.VMEM((rows, width), BF16), pltpu.VMEM((tokens, 128), F32), pltpu.VMEM((2, tokens, 128), F32),
            pltpu.VMEM((blocks, 2, 2, 2, rows, COLS), BF16), pltpu.VMEM((blocks, 2, 2, rows, COLS), BF16),
            pltpu.VMEM((blocks, 2, 2, rows, COLS), BF16), pltpu.VMEM((blocks, 2, rows, COLS), BF16),
            pltpu.VMEM((blocks, rows, COLS), F32), pltpu.VMEM((blocks, rows, COLS), BF16), pltpu.VMEM((blocks, rows, COLS), BF16),
            pltpu.SemaphoreType.DMA((2, 10, blocks)), pltpu.SemaphoreType.DMA((2, 10, blocks)),
            pltpu.SemaphoreType.DMA((blocks,)), pltpu.SemaphoreType.DMA((SLOTS,)), pltpu.SemaphoreType.DMA((SLOTS,)),
            pltpu.SemaphoreType.DMA((DSLOTS,)), pltpu.SemaphoreType.DMA],
        compiler_params=pltpu.CompilerParams(vmem_limit_bytes=LIM, collective_id=0, has_side_effects=True),
    )(o, ids, mids, gates, x, norm, router, wo, wg, wu, wd)


def solution(mesh):
    def local_step(x, k_cache, v_cache, positions, att_ids, mlp_ids, norm_att, w_kv, router_att, w_query, w_out, norm_mlp, router_mlp, w_gate, w_up, w_down):
        tokens, width = x.shape
        cache_shape = k_cache.shape
        heads, head_dim = cache_shape[2], cache_shape[3]
        half = np.arange(head_dim // 2, dtype=np.float64)
        freq = (ROPE_BASE ** (-(half * 2.0 / head_dim))).astype(np.float32)
        freq = np.concatenate([freq, freq])[None, :]
        wkv = w_kv.reshape(width, heads, 2, head_dim).transpose(0, 2, 1, 3).reshape(-1, head_dim)
        att, gates, keys_all, values_all = attention(
            positions, att_ids.T, positions[None, :], freq, norm_att[None, :], router_att.T, x, wkv, w_query,
            k_cache.reshape(-1, head_dim), v_cache.reshape(-1, head_dim))
        x_out = out_mlp(att, att_ids.T, mlp_ids.T, gates, x, norm_mlp[None, :], router_mlp.T, w_out, w_gate[0], w_up[0], w_down[0])
        return x_out, keys_all.reshape(cache_shape), values_all.reshape(cache_shape)

    token_spec = P('dp', None)
    cache_spec = P('dp', None, 'tp', None)
    expert_spec = P('tp', None, None)
    in_specs = (token_spec, cache_spec, cache_spec, P('dp'), token_spec, token_spec, P(), P(None, 'tp', None), P(), P(None, None, 'tp'), P(None, 'tp', None), P(), P(), expert_spec, expert_spec, expert_spec)
    out_specs = (token_spec, cache_spec, cache_spec)
    return jax.shard_map(local_step, mesh=mesh, in_specs=in_specs, out_specs=out_specs, check_vma=False)
```

```python
import jax
import jax.numpy as jnp
import numpy as np
from jax import lax
from jax.experimental import pallas as pl
from jax.experimental.pallas import tpu as pltpu
from jax.sharding import PartitionSpec as P

NORM_EPS = 1e-6
ROPE_BASE = 10000.0
F32 = jnp.float32
BF16 = jnp.bfloat16
MESH = pl.DeviceIdType.MESH
CHUNK = 32
LIM = 59 * 2**20
SUBS = 16


def rms_group(x_ref, norm_ref, out_ref, sl):
    v = x_ref[sl, :].astype(F32)
    inv = lax.rsqrt(jnp.mean(v * v, axis=-1, keepdims=True) + NORM_EPS)
    out_ref[sl, :] = (v * inv * norm_ref[...]).astype(BF16)


def spread(row):
    return jnp.broadcast_to(row.astype(F32), (128, row.shape[1])).T


def qa_kernel(pos_s, ids_ref, posr_ref, freq_ref, norm_ref, router_ref, x_hbm, wkv_hbm, wq_hbm, k_hbm, v_hbm,
              o_ref, gates_ref, kout_hbm, vout_hbm,
              x_ref, wkv_ref, x_sem, wkv_sem, h_s, wq_s, wkv_s, kbuf, vbuf, kn_s, vn_s, q_s, idb_s, posb_s, cos_s, sin_s, wq_sem, k_sem, v_sem, ko_sem, vo_sem):
    tokens = x_ref.shape[0]
    experts = wq_hbm.shape[0]
    chunks = tokens // CHUNK
    crow = CHUNK * 64
    per = chunks // experts

    def copies(c):
        sl = pl.ds(pl.multiple_of(c * crow, crow), crow)
        return (pltpu.make_async_copy(k_hbm.at[sl], kbuf.at[sl], k_sem.at[c]),
                pltpu.make_async_copy(v_hbm.at[sl], vbuf.at[sl], v_sem.at[c]))

    def out_copies(c):
        sl = pl.ds(pl.multiple_of(c * crow, crow), crow)
        return (pltpu.make_async_copy(kbuf.at[sl], kout_hbm.at[sl], ko_sem.at[c]),
                pltpu.make_async_copy(vbuf.at[sl], vout_hbm.at[sl], vo_sem.at[c]))

    def wq_copy(e):
        return pltpu.make_async_copy(wq_hbm.at[e], wq_s.at[e], wq_sem.at[e])

    x_copy = pltpu.make_async_copy(x_hbm, x_ref, x_sem)
    wkv_copy = pltpu.make_async_copy(wkv_hbm, wkv_ref, wkv_sem)
    x_copy.start()
    wkv_copy.start()
    r = lax.broadcasted_iota(jnp.int32, (256, 256), 0)
    swap = (lax.broadcasted_iota(jnp.int32, (256, 256), 1) == 4 * (r % 64) + r // 64).astype(F32).astype(BF16)

    x_copy.wait()
    wkv_copy.wait()
    steps = wkv_ref.shape[0] // 1024
    group = tokens // steps

    @pl.loop(0, steps)
    def _(i):
        wq_copy(i).start()
        for j in range(per):
            for cp in copies(i * per + j):
                cp.start()
        for j in range(4):
            part = jnp.dot(swap, wkv_ref[pl.ds(pl.multiple_of(i * 1024 + j * 256, 256), 256), :], preferred_element_type=F32).astype(BF16)
            for n in range(4):
                wkv_s[pl.ds(pl.multiple_of(i * 256 + j * 64, 64), 64), n * 128:(n + 1) * 128] = part[n * 64:(n + 1) * 64]
        rms_group(x_ref, norm_ref, h_s, pl.ds(pl.multiple_of(i * group, group), group))

    for k in range(2):
        idb_s[k] = spread(ids_ref[k:k + 1, :])
    pos = spread(posr_ref[...])
    posb_s[...] = pos.astype(jnp.int32)
    angle = pos * freq_ref[...]
    cos_s[...] = jnp.cos(angle)
    sin = jnp.sin(angle)
    sin_s[...] = jnp.where(lax.broadcasted_iota(jnp.int32, (tokens, 128), 1) < 64, -sin, sin)

    kv = jnp.dot(h_s[...], wkv_s[...], preferred_element_type=F32)
    for n in range(2):
        v = kv[:, n * 128:(n + 1) * 128]
        kn_s[n] = v * cos_s[...] + pltpu.roll(v, 64, 1) * sin_s[...]
        vn_s[n] = kv[:, 256 + n * 128:256 + (n + 1) * 128]
    logits = lax.dot_general(h_s[...], router_ref[...], (((1,), (1,)), ((), ())), preferred_element_type=F32)
    lane = lax.broadcasted_iota(jnp.int32, logits.shape, 1).astype(F32)
    hit0, hit1 = lane == idb_s[0, :, 0:experts], lane == idb_s[1, :, 0:experts]
    l0 = jnp.sum(jnp.where(hit0, logits, 0.0), axis=1, keepdims=True)
    l1 = jnp.sum(jnp.where(hit1, logits, 0.0), axis=1, keepdims=True)
    top = jnp.maximum(l0, l1)
    e0, e1 = jnp.exp(l0 - top), jnp.exp(l1 - top)
    inv = 1.0 / (e0 + e1)
    gates_ref[...] = jnp.where(lane == 0.0, e0 * inv, e1 * inv)

    r16 = lax.broadcasted_iota(jnp.int32, (16, 128), 0)
    odd16, pair16 = r16 % 2 == 1, r16 // 2

    @pl.loop(0, experts)
    def _(e):
        wq_copy(e).wait()
        for i in range(per):
            for cp in copies(e * per + i):
                cp.wait()
        q = jnp.dot(h_s[...], wq_s[e], preferred_element_type=F32)
        for t in range(per * CHUNK):
            tok = e * (per * CHUNK) + t
            p = pos_s[tok]
            at = pl.ds(pl.multiple_of(tok * 64 + (p // 8) * 16, 16), 16)
            here = pair16 == p % 8
            for buf, new in ((kbuf, kn_s), (vbuf, vn_s)):
                a = jnp.broadcast_to(new[0, pl.ds(tok, 1), :], (16, 128))
                b = jnp.broadcast_to(new[1, pl.ds(tok, 1), :], (16, 128))
                buf[at, :] = jnp.where(here, jnp.where(odd16, b, a), buf[at, :].astype(F32)).astype(BF16)
        for i in range(per):
            for cp in out_copies(e * per + i):
                cp.start()
        for k in range(2):
            h3 = (idb_s[k] == e.astype(F32)).reshape(tokens // 8, 8, 128)
            for n in range(2):
                part = q[:, n * 128:(n + 1) * 128].reshape(tokens // 8, 8, 128)
                q_s[:, 2 * n + k] = jnp.where(h3, part, q_s[:, 2 * n + k])

    cos3, sin3 = cos_s[...].reshape(tokens // 8, 8, 128), sin_s[...].reshape(tokens // 8, 8, 128)
    for j in range(4):
        v = q_s[:, j]
        q_s[:, j] = v * cos3 + pltpu.roll(v, 64, 2) * sin3

    col = lax.broadcasted_iota(jnp.int32, (8, 512), 1)
    row = lax.broadcasted_iota(jnp.int32, (8, 512), 0)
    slots = [jnp.where((col // 64 == row) & (col % 2 == n), (col % 64) // 2, 1 << 20) for n in range(2)]

    @pl.loop(0, tokens // (8 * SUBS))
    def _(g):
        base = g * SUBS
        rows = [pl.ds(pl.multiple_of((base + s) * 512, 512), 512) for s in range(SUBS)]
        toks = [pl.ds(pl.multiple_of((base + s) * 8, 8), 8) for s in range(SUBS)]
        scores = [lax.dot_general(q_s[base + s].reshape(32, 128).astype(BF16), kbuf[rows[s], :], (((1,), (1,)), ((), ())),
                                  preferred_element_type=F32) for s in range(SUBS)]
        weights = []
        for s in range(SUBS):
            here = jnp.concatenate([posb_s[toks[s], :]] * 4, axis=1)
            vis = [sl <= here for sl in slots]
            mask = jnp.concatenate([vis[0], vis[0], vis[1], vis[1]], axis=0)
            sc = jnp.where(mask, scores[s] * 128 ** -0.5, -1e30)
            ex = jnp.exp(sc - jnp.max(sc, axis=1, keepdims=True))
            weights.append((ex * (1.0 / jnp.sum(ex, axis=1, keepdims=True))).astype(BF16))
        outs = [jnp.dot(weights[s], vbuf[rows[s], :], preferred_element_type=F32) for s in range(SUBS)]
        for s in range(SUBS):
            for k in range(2):
                for n in range(2):
                    o_ref[k, toks[s], n * 128:(n + 1) * 128] = outs[s][(2 * n + k) * 8:(2 * n + k + 1) * 8]

    @pl.loop(0, chunks)
    def _(c):
        for cp in out_copies(c):
            cp.wait()


def attention(pos, ids, posr, freq, norm, router, x, wkv, wq, kc, vc):
    tokens, width = x.shape
    experts, _, qw = wq.shape
    vmem = pl.BlockSpec(memory_space=pltpu.VMEM)
    hbm = pl.BlockSpec(memory_space=pl.ANY)
    chunks = tokens // CHUNK
    return pl.pallas_call(
        qa_kernel,
        name="qkv_attention",
        out_shape=(pltpu.VMEM((2, tokens, qw), F32), jax.ShapeDtypeStruct((tokens, experts), F32),
                   jax.ShapeDtypeStruct(kc.shape, BF16), jax.ShapeDtypeStruct(vc.shape, BF16)),
        in_specs=[pl.BlockSpec(memory_space=pltpu.SMEM)] + [vmem] * 5 + [hbm] * 5,
        out_specs=(vmem, vmem, hbm, hbm),
        scratch_shapes=[
            pltpu.VMEM(x.shape, BF16), pltpu.VMEM(wkv.shape, BF16), pltpu.SemaphoreType.DMA, pltpu.SemaphoreType.DMA,
            pltpu.VMEM((tokens, width), BF16), pltpu.VMEM(wq.shape, BF16), pltpu.VMEM((width, 512), BF16),
            pltpu.VMEM(kc.shape, BF16), pltpu.VMEM(vc.shape, BF16),
            pltpu.VMEM((2, tokens, 128), F32), pltpu.VMEM((2, tokens, 128), F32),
            pltpu.VMEM((tokens // 8, 4, 8, 128), F32), pltpu.VMEM((2, tokens, 128), F32),
            pltpu.VMEM((tokens, 128), jnp.int32), pltpu.VMEM((tokens, 128), F32), pltpu.VMEM((tokens, 128), F32),
            pltpu.SemaphoreType.DMA((experts,))] + [pltpu.SemaphoreType.DMA((chunks,))] * 4,
        compiler_params=pltpu.CompilerParams(vmem_limit_bytes=60 * 2**20),
    )(pos, ids, posr, freq, norm, router, x, wkv, wq, kc, vc)


D2D, RS1, RS2, AGX, AGY, AGS, FWD, FXS, FYS, FDS = range(10)
COLS = 256
FB = 512
SLOTS = 4
DSLOTS = 4
DIRECT = 2
NROWS = 512


def om_kernel(o_ref, ids_ref, mids_ref, gates_ref, x_hbm, norm_ref, router_ref, wo_hbm, wg_hbm, wu_hbm, wd_hbm,
              out_ref,
              wo_s, wg_s, wu_s, wd_s, a_s, u_s, xo_s, xm_s, wb_s, g_s, mid_s, p_s, d_s, s1_s, r1_s, own_s, s2_s, r2_s,
              ssem, rsem, wo_sem, g_sem, up_sem, wd_sem, x_sem):
    tokens, width = u_s.shape
    experts = wo_hbm.shape[0]
    ffn = wg_hbm.shape[1]
    rows = tokens // 8
    blocks = width // COLS
    fblocks = ffn // FB
    dp, me = lax.axis_index("dp"), lax.axis_index("tp")
    c, xx, yy = me % 2, (me // 2) % 2, me // 4
    sib, xn, yn = me + 1 - 2 * c, me + 2 - 4 * xx, me + 4 - 8 * yy
    dn = xn + 4 - 8 * yy

    def cols(b):
        return pl.ds(pl.multiple_of(b * COLS, COLS), COLS)

    def wo_copy(b):
        return pltpu.make_async_copy(wo_hbm.at[:, :, cols(b)], wo_s.at[b], wo_sem.at[b])

    def up_copies(f, slot):
        cs = pl.ds(pl.multiple_of(f * FB, FB), FB)
        return (pltpu.make_async_copy(wg_hbm.at[:, cs], wg_s.at[slot], g_sem.at[slot]),
                pltpu.make_async_copy(wu_hbm.at[:, cs], wu_s.at[slot], up_sem.at[slot]))

    def wd_copy(d):
        return pltpu.make_async_copy(wd_hbm.at[:, cols(d)], wd_s.at[d % DSLOTS], wd_sem.at[d % DSLOTS])

    mine = pl.ds(pl.multiple_of(me * rows, rows), rows)
    x_copy = pltpu.make_async_copy(x_hbm.at[mine], xo_s, x_sem)
    for b in range(2):
        wo_copy(b).start()
    x_copy.start()

    barrier = pltpu.get_barrier_semaphore()
    for other in (sib, xn, yn, dn):
        pl.semaphore_signal(barrier, inc=1, device_id=(dp, other), device_id_type=MESH)

    id0, id1 = spread(ids_ref[0:1, :]), spread(ids_ref[1:2, :])
    for k in range(2):
        mid_s[k] = spread(mids_ref[k:k + 1, :])
    for k, ids in enumerate((id0, id1)):
        for e in range(experts):
            for n in range(2):
                at = (k * experts + e) * COLS + n * 128
                a_s[:, at:at + 128] = jnp.where(ids == e, o_ref[k, :, n * 128:(n + 1) * 128], 0.0).astype(BF16)
        g_s[k] = jnp.broadcast_to(gates_ref[:, k:k + 1], (tokens, 128))

    @pl.loop(2, blocks)
    def _(b):
        wo_copy(b).start()

    x_copy.wait()
    pl.semaphore_wait(barrier, 4)

    def all_reduce(r, produce, lead, dest, finish):
        def remote(stage, b, src, dst, to):
            return pltpu.make_async_remote_copy(src_ref=src, dst_ref=dst, send_sem=ssem.at[r, stage, b], recv_sem=rsem.at[r, stage, b],
                                                device_id=(dp, to), device_id_type=MESH)

        def at(dev, b):
            return dest.at[pl.ds(pl.multiple_of(dev * rows, rows), rows), pl.ds(pl.multiple_of(b * COLS, COLS), COLS)]

        def push(stage, b, dev, to):
            return remote(stage, b, at(dev, b), at(dev, b), to)

        def d2d(b, odd):
            return remote(D2D, b, p_s.at[b, :, :, 1 - c], d_s.at[b], sib)

        def rs1(b, odd):
            src = s1_s.at[b, 1 - yy] if odd else s1_s.at[b, :, 1 - xx]
            return remote(RS1, b, src, r1_s.at[b], yn if odd else xn)

        def rs2(b, odd):
            return remote(RS2, b, s2_s.at[b], r2_s.at[b], xn if odd else yn)

        def agx(b, odd):
            return push(AGX, b, me, xn)

        def agy(b, odd):
            return push(AGY, b, me, yn)

        def ags(b, odd):
            return push(AGS, b, me, sib)

        def fwd(b, odd):
            return push(FWD, b, yn, xn) if odd else push(FWD, b, xn, yn)

        def far(b, odd):
            return push(FWD, b, me, dn)

        def fxs(b, odd):
            return push(FXS, b, xn, sib)

        def fys(b, odd):
            return push(FYS, b, yn, sib)

        def fds(b, odd):
            return push(FDS, b, dn, sib)

        def st0(b, odd):
            produce(b)
            d2d(b, odd).start()

        def st1(b, odd):
            d2d(b, odd).wait_recv()
            for j in range(2):
                for i in range(2):
                    s1_s[b, j, i] = (p_s[b, j, i, c].astype(F32) + d_s[b, j, i].astype(F32)).astype(BF16)
            rs1(b, odd).start()

        def st2(b, odd):
            rs1(b, odd).wait_recv()
            keep = s1_s[b, yy, xx].astype(F32)
            if odd:
                keep = keep + r1_s[b, xx].astype(F32)
                give = s1_s[b, yy, 1 - xx].astype(F32) + r1_s[b, 1 - xx].astype(F32)
            else:
                keep = keep + r1_s[b, yy].astype(F32)
                give = s1_s[b, 1 - yy, xx].astype(F32) + r1_s[b, 1 - yy].astype(F32)
            s2_s[b] = give.astype(BF16)
            rs2(b, odd).start()
            own_s[b] = keep

        def st3(b, odd):
            rs2(b, odd).wait_recv()
            finish(b, own_s[b] + r2_s[b].astype(F32))
            agx(b, odd).start()
            agy(b, odd).start()

            @pl.when(b >= blocks - DIRECT)
            def _():
                far(b, odd).start()

            ags(b, odd).start()

        def st4(b, odd):
            agx(b, odd).wait_recv()
            agy(b, odd).wait_recv()

            @pl.when(b < blocks - DIRECT)
            def _():
                fwd(b, odd).start()

            fxs(b, odd).start()
            fys(b, odd).start()

        def st5(b, odd):
            far(b, odd).wait_recv()
            fds(b, odd).start()

        def st6(b, odd):
            for make in (ags, fxs, fys, fds):
                make(b, odd).wait_recv()

        stages = (st0, st1, st2, st3, st4, st5, st6)

        @pl.loop(0, (blocks + lead[-1] + 1) // 2)
        def _(t):
            for half in range(2):
                for stage, lag in zip(stages, lead):
                    b = 2 * t + half - lag

                    @pl.when((b >= 0) & (b < blocks))
                    def _():
                        stage(b, (half - lag) % 2)

        @pl.loop(0, blocks)
        def _(b):
            for make in (d2d, rs1, rs2, agx, agy, ags, far, fxs, fys, fds):
                make(b, 0).wait_send()

    def put(b, value):
        p_s[b] = value.astype(BF16).reshape(2, 2, 2, rows, COLS)

    def att_block(b):
        wo_copy(b).wait()
        w = wo_s[b].reshape(experts * COLS, COLS)
        total = None
        for k in range(2):
            part = jnp.dot(a_s[:, k * experts * COLS:(k + 1) * experts * COLS], w, preferred_element_type=F32)
            part = part * jnp.concatenate([g_s[k]] * 2, axis=1)
            total = part if total is None else total + part
        put(b, total)

        @pl.when(b < SLOTS)
        def _():
            for cp in up_copies(b, b):
                cp.start()

        @pl.when((b >= SLOTS) & (b < SLOTS + DSLOTS))
        def _():
            wd_copy(b - SLOTS).start()

    def att_finish(b, total):
        cs = cols(b)
        mid = (xo_s[:, cs].astype(F32) + total).astype(BF16)
        xm_s[:, cs] = mid
        u_s[mine, cs] = mid

    all_reduce(0, att_block, (0, 1, 3, 5, 7, 9, 11), u_s, att_finish)
    here = me.astype(F32)
    lane = lax.broadcasted_iota(jnp.int32, (NROWS, experts), 1).astype(F32)

    @pl.loop(0, tokens // NROWS)
    def _(i):
        sl = pl.ds(pl.multiple_of(i * NROWS, NROWS), NROWS)
        rms_group(u_s, norm_ref, u_s, sl)
        logits = lax.dot_general(u_s[sl, :], router_ref[...], (((1,), (1,)), ((), ())), preferred_element_type=F32)
        id2, id3 = mid_s[0, sl, :], mid_s[1, sl, :]
        l0 = jnp.sum(jnp.where(lane == id2[:, 0:experts], logits, 0.0), axis=1, keepdims=True)
        l1 = jnp.sum(jnp.where(lane == id3[:, 0:experts], logits, 0.0), axis=1, keepdims=True)
        top = jnp.maximum(l0, l1)
        e0, e1 = jnp.exp(l0 - top), jnp.exp(l1 - top)
        inv = 1.0 / (e0 + e1)
        wb_s[sl, :] = jnp.where(id2 == here, e0 * inv, 0.0) + jnp.where(id3 == here, e1 * inv, 0.0)

    @pl.loop(0, fblocks)
    def _(f):
        slot = f % SLOTS
        for cp in up_copies(f, slot):
            cp.wait()
        g = jnp.dot(u_s[...], wg_s[slot], preferred_element_type=F32)
        up = jnp.dot(u_s[...], wu_s[slot], preferred_element_type=F32)
        a_s[:, pl.ds(pl.multiple_of(f * FB, FB), FB)] = (g * (1.0 / (1.0 + jnp.exp(-g))) * up).astype(BF16)

        @pl.when(f + SLOTS < fblocks)
        def _():
            for cp in up_copies(f + SLOTS, slot):
                cp.start()

    def down_block(b):
        wd_copy(b).wait()
        y = jnp.dot(a_s[...], wd_s[b % DSLOTS], preferred_element_type=F32)
        put(b, y * jnp.concatenate([wb_s[...]] * 2, axis=1))

        @pl.when(b + DSLOTS < blocks)
        def _():
            wd_copy(b + DSLOTS).start()

    def down_finish(b, total):
        cs = cols(b)
        out_ref[mine, cs] = (xm_s[:, cs].astype(F32) + total).astype(BF16)

    all_reduce(1, down_block, (0, 1, 3, 5, 7, 9, 11), out_ref, down_finish)


def out_mlp(o, ids, mids, gates, x, norm, router, wo, wg, wu, wd):
    tokens, width = x.shape
    experts = wo.shape[0]
    rows = tokens // 8
    blocks = width // COLS
    vmem = pl.BlockSpec(memory_space=pltpu.VMEM)
    hbm = pl.BlockSpec(memory_space=pl.ANY)
    return pl.pallas_call(
        om_kernel,
        name="out_mlp",
        out_shape=pltpu.VMEM((tokens, width), BF16),
        in_specs=[vmem] * 4 + [hbm] + [vmem] * 2 + [hbm] * 4,
        out_specs=vmem,
        scratch_shapes=[
            pltpu.VMEM((blocks, experts, COLS, COLS), BF16),
            pltpu.VMEM((SLOTS, width, FB), BF16), pltpu.VMEM((SLOTS, width, FB), BF16),
            pltpu.VMEM((DSLOTS, wd.shape[0], COLS), BF16),
            pltpu.VMEM((tokens, wd.shape[0]), BF16), pltpu.VMEM((tokens, width), BF16),
            pltpu.VMEM((rows, width), BF16), pltpu.VMEM((rows, width), BF16), pltpu.VMEM((tokens, 128), F32), pltpu.VMEM((2, tokens, 128), F32), pltpu.VMEM((2, tokens, 128), F32),
            pltpu.VMEM((blocks, 2, 2, 2, rows, COLS), BF16), pltpu.VMEM((blocks, 2, 2, rows, COLS), BF16),
            pltpu.VMEM((blocks, 2, 2, rows, COLS), BF16), pltpu.VMEM((blocks, 2, rows, COLS), BF16),
            pltpu.VMEM((blocks, rows, COLS), F32), pltpu.VMEM((blocks, rows, COLS), BF16), pltpu.VMEM((blocks, rows, COLS), BF16),
            pltpu.SemaphoreType.DMA((2, 10, blocks)), pltpu.SemaphoreType.DMA((2, 10, blocks)),
            pltpu.SemaphoreType.DMA((blocks,)), pltpu.SemaphoreType.DMA((SLOTS,)), pltpu.SemaphoreType.DMA((SLOTS,)),
            pltpu.SemaphoreType.DMA((DSLOTS,)), pltpu.SemaphoreType.DMA],
        compiler_params=pltpu.CompilerParams(vmem_limit_bytes=LIM, collective_id=0, has_side_effects=True),
    )(o, ids, mids, gates, x, norm, router, wo, wg, wu, wd)


def solution(mesh):
    def local_step(x, k_cache, v_cache, positions, att_ids, mlp_ids, norm_att, w_kv, router_att, w_query, w_out, norm_mlp, router_mlp, w_gate, w_up, w_down):
        tokens, width = x.shape
        cache_shape = k_cache.shape
        heads, head_dim = cache_shape[2], cache_shape[3]
        half = np.arange(head_dim // 2, dtype=np.float64)
        freq = (ROPE_BASE ** (-(half * 2.0 / head_dim))).astype(np.float32)
        freq = np.concatenate([freq, freq])[None, :]
        wkv = w_kv.reshape(width, heads, 2, head_dim).transpose(0, 2, 1, 3).reshape(-1, head_dim)
        att, gates, keys_all, values_all = attention(
            positions, att_ids.T, positions[None, :], freq, norm_att[None, :], router_att.T, x, wkv, w_query,
            k_cache.reshape(-1, head_dim), v_cache.reshape(-1, head_dim))
        att = pltpu.with_memory_space_constraint(att, pltpu.VMEM)
        x_out = out_mlp(att, att_ids.T, mlp_ids.T, gates, x, norm_mlp[None, :], router_mlp.T, w_out, w_gate[0], w_up[0], w_down[0])
        return x_out, keys_all.reshape(cache_shape), values_all.reshape(cache_shape)

    token_spec = P('dp', None)
    cache_spec = P('dp', None, 'tp', None)
    expert_spec = P('tp', None, None)
    in_specs = (token_spec, cache_spec, cache_spec, P('dp'), token_spec, token_spec, P(), P(None, 'tp', None), P(), P(None, None, 'tp'), P(None, 'tp', None), P(), P(), expert_spec, expert_spec, expert_spec)
    out_specs = (token_spec, cache_spec, cache_spec)
    return jax.shard_map(local_step, mesh=mesh, in_specs=in_specs, out_specs=out_specs, check_vma=False)
```

```python
import jax
import jax.numpy as jnp
import numpy as np
from jax import lax
from jax.experimental import pallas as pl
from jax.experimental.pallas import tpu as pltpu
from jax.sharding import PartitionSpec as P

NORM_EPS = 1e-6
ROPE_BASE = 10000.0
F32 = jnp.float32
BF16 = jnp.bfloat16
MESH = pl.DeviceIdType.MESH
CHUNK = 32
LIM = 59 * 2**20
SUBS = 16


def rms_group(x_ref, norm_ref, out_ref, sl):
    v = x_ref[sl, :].astype(F32)
    inv = lax.rsqrt(jnp.mean(v * v, axis=-1, keepdims=True) + NORM_EPS)
    out_ref[sl, :] = (v * inv * norm_ref[...]).astype(BF16)


def spread(row):
    return jnp.broadcast_to(row.astype(F32), (128, row.shape[1])).T


def by_half(v):
    part = v.shape[0] // 16
    return jnp.concatenate([v[(2 * j + h) * part:(2 * j + h + 1) * part] for h in range(2) for j in range(8)], axis=0)


def qa_kernel(pos_s, ids_ref, posr_ref, freq_ref, norm_ref, router_ref, x_hbm, wkv_hbm, wq_hbm, k_hbm, v_hbm,
              o_ref, gates_ref, kout_hbm, vout_hbm,
              x_ref, wkv_ref, x_sem, wkv_sem, h_s, wq_s, wkv_s, kbuf, vbuf, kn_s, vn_s, q_s, idb_s, posb_s, cos_s, sin_s, wq_sem, k_sem, v_sem, ko_sem, vo_sem):
    tokens = x_ref.shape[0]
    experts = wq_hbm.shape[0]
    chunks = tokens // CHUNK
    crow = CHUNK * 64
    per = chunks // experts

    def copies(c):
        sl = pl.ds(pl.multiple_of(c * crow, crow), crow)
        return (pltpu.make_async_copy(k_hbm.at[sl], kbuf.at[sl], k_sem.at[c]),
                pltpu.make_async_copy(v_hbm.at[sl], vbuf.at[sl], v_sem.at[c]))

    def out_copies(c):
        sl = pl.ds(pl.multiple_of(c * crow, crow), crow)
        return (pltpu.make_async_copy(kbuf.at[sl], kout_hbm.at[sl], ko_sem.at[c]),
                pltpu.make_async_copy(vbuf.at[sl], vout_hbm.at[sl], vo_sem.at[c]))

    def wq_copy(e):
        return pltpu.make_async_copy(wq_hbm.at[e], wq_s.at[e], wq_sem.at[e])

    x_copy = pltpu.make_async_copy(x_hbm, x_ref, x_sem)
    wkv_copy = pltpu.make_async_copy(wkv_hbm, wkv_ref, wkv_sem)
    x_copy.start()
    wkv_copy.start()
    r = lax.broadcasted_iota(jnp.int32, (256, 256), 0)
    swap = (lax.broadcasted_iota(jnp.int32, (256, 256), 1) == 4 * (r % 64) + r // 64).astype(F32).astype(BF16)

    x_copy.wait()
    wkv_copy.wait()
    steps = wkv_ref.shape[0] // 1024
    group = tokens // steps

    @pl.loop(0, steps)
    def _(i):
        wq_copy(i).start()
        for j in range(per):
            for cp in copies(i * per + j):
                cp.start()
        for j in range(4):
            part = jnp.dot(swap, wkv_ref[pl.ds(pl.multiple_of(i * 1024 + j * 256, 256), 256), :], preferred_element_type=F32).astype(BF16)
            for n in range(4):
                wkv_s[pl.ds(pl.multiple_of(i * 256 + j * 64, 64), 64), n * 128:(n + 1) * 128] = part[n * 64:(n + 1) * 64]
        rms_group(x_ref, norm_ref, h_s, pl.ds(pl.multiple_of(i * group, group), group))

    for k in range(2):
        idb_s[k] = spread(ids_ref[k:k + 1, :])
    pos = spread(posr_ref[...])
    posb_s[...] = pos.astype(jnp.int32)
    angle = pos * freq_ref[...]
    cos_s[...] = jnp.cos(angle)
    sin = jnp.sin(angle)
    sin_s[...] = jnp.where(lax.broadcasted_iota(jnp.int32, (tokens, 128), 1) < 64, -sin, sin)

    kv = jnp.dot(h_s[...], wkv_s[...], preferred_element_type=F32)
    for n in range(2):
        v = kv[:, n * 128:(n + 1) * 128]
        kn_s[n] = v * cos_s[...] + pltpu.roll(v, 64, 1) * sin_s[...]
        vn_s[n] = kv[:, 256 + n * 128:256 + (n + 1) * 128]
    logits = lax.dot_general(h_s[...], router_ref[...], (((1,), (1,)), ((), ())), preferred_element_type=F32)
    lane = lax.broadcasted_iota(jnp.int32, logits.shape, 1).astype(F32)
    hit0, hit1 = lane == idb_s[0, :, 0:experts], lane == idb_s[1, :, 0:experts]
    l0 = jnp.sum(jnp.where(hit0, logits, 0.0), axis=1, keepdims=True)
    l1 = jnp.sum(jnp.where(hit1, logits, 0.0), axis=1, keepdims=True)
    top = jnp.maximum(l0, l1)
    e0, e1 = jnp.exp(l0 - top), jnp.exp(l1 - top)
    inv = 1.0 / (e0 + e1)
    gates_ref[...] = by_half(jnp.where(lane == 0.0, e0 * inv, e1 * inv))

    r16 = lax.broadcasted_iota(jnp.int32, (16, 128), 0)
    odd16, pair16 = r16 % 2 == 1, r16 // 2

    @pl.loop(0, experts)
    def _(e):
        wq_copy(e).wait()
        for i in range(per):
            for cp in copies(e * per + i):
                cp.wait()
        q = jnp.dot(h_s[...], wq_s[e], preferred_element_type=F32)
        for t in range(per * CHUNK):
            tok = e * (per * CHUNK) + t
            p = pos_s[tok]
            at = pl.ds(pl.multiple_of(tok * 64 + (p // 8) * 16, 16), 16)
            here = pair16 == p % 8
            for buf, new in ((kbuf, kn_s), (vbuf, vn_s)):
                a = jnp.broadcast_to(new[0, pl.ds(tok, 1), :], (16, 128))
                b = jnp.broadcast_to(new[1, pl.ds(tok, 1), :], (16, 128))
                buf[at, :] = jnp.where(here, jnp.where(odd16, b, a), buf[at, :].astype(F32)).astype(BF16)
        for i in range(per):
            for cp in out_copies(e * per + i):
                cp.start()
        for k in range(2):
            h3 = (idb_s[k] == e.astype(F32)).reshape(tokens // 8, 8, 128)
            for n in range(2):
                part = q[:, n * 128:(n + 1) * 128].reshape(tokens // 8, 8, 128)
                q_s[:, 2 * n + k] = jnp.where(h3, part, q_s[:, 2 * n + k])

    cos3, sin3 = cos_s[...].reshape(tokens // 8, 8, 128), sin_s[...].reshape(tokens // 8, 8, 128)
    for j in range(4):
        v = q_s[:, j]
        q_s[:, j] = v * cos3 + pltpu.roll(v, 64, 2) * sin3

    col = lax.broadcasted_iota(jnp.int32, (8, 512), 1)
    row = lax.broadcasted_iota(jnp.int32, (8, 512), 0)
    slots = [jnp.where((col // 64 == row) & (col % 2 == n), (col % 64) // 2, 1 << 20) for n in range(2)]

    @pl.loop(0, tokens // (8 * SUBS))
    def _(g):
        base = g * SUBS
        rows = [pl.ds(pl.multiple_of((base + s) * 512, 512), 512) for s in range(SUBS)]
        toks = [pl.ds(pl.multiple_of((base + s) * 8, 8), 8) for s in range(SUBS)]
        dest = [pl.ds(pl.multiple_of(((s % 8) // 4 * 32 + (base // 8 + s // 8) * 4 + s % 4) * 8, 8), 8) for s in range(SUBS)]
        scores = [lax.dot_general(q_s[base + s].reshape(32, 128).astype(BF16), kbuf[rows[s], :], (((1,), (1,)), ((), ())),
                                  preferred_element_type=F32) for s in range(SUBS)]
        weights = []
        for s in range(SUBS):
            here = jnp.concatenate([posb_s[toks[s], :]] * 4, axis=1)
            vis = [sl <= here for sl in slots]
            mask = jnp.concatenate([vis[0], vis[0], vis[1], vis[1]], axis=0)
            sc = jnp.where(mask, scores[s] * 128 ** -0.5, -1e30)
            ex = jnp.exp(sc - jnp.max(sc, axis=1, keepdims=True))
            weights.append((ex * (1.0 / jnp.sum(ex, axis=1, keepdims=True))).astype(BF16))
        outs = [jnp.dot(weights[s], vbuf[rows[s], :], preferred_element_type=F32) for s in range(SUBS)]
        for s in range(SUBS):
            for k in range(2):
                for n in range(2):
                    o_ref[k, dest[s], n * 128:(n + 1) * 128] = outs[s][(2 * n + k) * 8:(2 * n + k + 1) * 8]

    @pl.loop(0, chunks)
    def _(c):
        for cp in out_copies(c):
            cp.wait()


def attention(pos, ids, posr, freq, norm, router, x, wkv, wq, kc, vc):
    tokens, width = x.shape
    experts, _, qw = wq.shape
    vmem = pl.BlockSpec(memory_space=pltpu.VMEM)
    hbm = pl.BlockSpec(memory_space=pl.ANY)
    chunks = tokens // CHUNK
    return pl.pallas_call(
        qa_kernel,
        name="qkv_attention",
        out_shape=(pltpu.VMEM((2, tokens, qw), F32), jax.ShapeDtypeStruct((tokens, experts), F32),
                   jax.ShapeDtypeStruct(kc.shape, BF16), jax.ShapeDtypeStruct(vc.shape, BF16)),
        in_specs=[pl.BlockSpec(memory_space=pltpu.SMEM)] + [vmem] * 5 + [hbm] * 5,
        out_specs=(vmem, vmem, hbm, hbm),
        scratch_shapes=[
            pltpu.VMEM(x.shape, BF16), pltpu.VMEM(wkv.shape, BF16), pltpu.SemaphoreType.DMA, pltpu.SemaphoreType.DMA,
            pltpu.VMEM((tokens, width), BF16), pltpu.VMEM(wq.shape, BF16), pltpu.VMEM((width, 512), BF16),
            pltpu.VMEM(kc.shape, BF16), pltpu.VMEM(vc.shape, BF16),
            pltpu.VMEM((2, tokens, 128), F32), pltpu.VMEM((2, tokens, 128), F32),
            pltpu.VMEM((tokens // 8, 4, 8, 128), F32), pltpu.VMEM((2, tokens, 128), F32),
            pltpu.VMEM((tokens, 128), jnp.int32), pltpu.VMEM((tokens, 128), F32), pltpu.VMEM((tokens, 128), F32),
            pltpu.SemaphoreType.DMA((experts,))] + [pltpu.SemaphoreType.DMA((chunks,))] * 4,
        compiler_params=pltpu.CompilerParams(vmem_limit_bytes=60 * 2**20),
    )(pos, ids, posr, freq, norm, router, x, wkv, wq, kc, vc)


D2D, RS1, RS2, AGX, AGY, AGS, FWD, FXS, FYS, FDS = range(10)
COLS = 512
PAIR = 256
FB = 512
SLOTS = 4
DSLOTS = 2
DIRECT = 2


def om_kernel(o_ref, ids_ref, mids_ref, gates_ref, x_hbm, norm_ref, router_ref, wo_hbm, wg_hbm, wu_hbm, wd_hbm,
              out_ref,
              wo_s, wg_s, wu_s, wd_s, a_s, u_s, xo_s, xm_s, wb_s, g_s, mid_s, p_s, d_s, s1_s, r1_s, own_s, s2_s, r2_s,
              ssem, rsem, wo_sem, g_sem, up_sem, wd_sem, x_sem):
    tokens, width = u_s.shape
    experts = wo_hbm.shape[0]
    ffn = wg_hbm.shape[1]
    rows = tokens // 8
    part = rows // 2
    side = tokens // 2
    wides = width // COLS
    blocks = 2 * wides
    fblocks = ffn // FB
    dp, me = lax.axis_index("dp"), lax.axis_index("tp")
    c, xx, yy = me % 2, (me // 2) % 2, me // 4
    sib, xn, yn = me + 1 - 2 * c, me + 2 - 4 * xx, me + 4 - 8 * yy
    dn = xn + 4 - 8 * yy

    def cols(b):
        return pl.ds(pl.multiple_of(b * COLS, COLS), COLS)

    def wo_copy(b):
        return pltpu.make_async_copy(wo_hbm.at[:, :, cols(b)], wo_s.at[b], wo_sem.at[b])

    def up_copies(f, slot):
        cs = pl.ds(pl.multiple_of(f * FB, FB), FB)
        return (pltpu.make_async_copy(wg_hbm.at[:, cs], wg_s.at[slot], g_sem.at[slot]),
                pltpu.make_async_copy(wu_hbm.at[:, cs], wu_s.at[slot], up_sem.at[slot]))

    def wd_copy(d):
        return pltpu.make_async_copy(wd_hbm.at[:, cols(d)], wd_s.at[d % DSLOTS], wd_sem.at[d % DSLOTS])

    mine = pl.ds(pl.multiple_of(me * rows, rows), rows)
    x_copy = pltpu.make_async_copy(x_hbm.at[mine], xo_s, x_sem)
    wo_copy(0).start()
    x_copy.start()

    barrier = pltpu.get_barrier_semaphore()
    for other in (sib, xn, yn, dn):
        pl.semaphore_signal(barrier, inc=1, device_id=(dp, other), device_id_type=MESH)

    id0, id1 = by_half(spread(ids_ref[0:1, :])), by_half(spread(ids_ref[1:2, :]))
    for k in range(2):
        mid_s[k] = by_half(spread(mids_ref[k:k + 1, :]))
    for k, ids in enumerate((id0, id1)):
        for e in range(experts):
            for n in range(2):
                at = (k * experts + e) * PAIR + n * 128
                a_s[:, at:at + 128] = jnp.where(ids == e, o_ref[k, :, n * 128:(n + 1) * 128], 0.0).astype(BF16)
        g_s[k] = jnp.broadcast_to(gates_ref[:, k:k + 1], (tokens, 128))

    @pl.loop(1, wides)
    def _(b):
        wo_copy(b).start()

    x_copy.wait()
    pl.semaphore_wait(barrier, 4)

    def all_reduce(r, produce, lead, dest, where, finish, extra=None):
        def remote(stage, b, src, dst, to):
            return pltpu.make_async_remote_copy(src_ref=src, dst_ref=dst, send_sem=ssem.at[r, stage, b], recv_sem=rsem.at[r, stage, b],
                                                device_id=(dp, to), device_id_type=MESH)

        def at(dev, b):
            row, col = where(dev, b)
            return dest.at[row, col]

        def push(stage, b, dev, to):
            return remote(stage, b, at(dev, b), at(dev, b), to)

        def d2d(b, odd):
            return remote(D2D, b, p_s.at[b, :, :, 1 - c], d_s.at[b], sib)

        def rs1(b, odd):
            src = s1_s.at[b, 1 - yy] if odd else s1_s.at[b, :, 1 - xx]
            return remote(RS1, b, src, r1_s.at[b], yn if odd else xn)

        def rs2(b, odd):
            return remote(RS2, b, s2_s.at[b], r2_s.at[b], xn if odd else yn)

        def agx(b, odd):
            return push(AGX, b, me, xn)

        def agy(b, odd):
            return push(AGY, b, me, yn)

        def ags(b, odd):
            return push(AGS, b, me, sib)

        def fwd(b, odd):
            return push(FWD, b, yn, xn) if odd else push(FWD, b, xn, yn)

        def far(b, odd):
            return push(FWD, b, me, dn)

        def fxs(b, odd):
            return push(FXS, b, xn, sib)

        def fys(b, odd):
            return push(FYS, b, yn, sib)

        def fds(b, odd):
            return push(FDS, b, dn, sib)

        def st0(b, odd):
            produce(b)
            d2d(b, odd).start()

        def st1(b, odd):
            d2d(b, odd).wait_recv()
            for j in range(2):
                for i in range(2):
                    s1_s[b, j, i] = (p_s[b, j, i, c].astype(F32) + d_s[b, j, i].astype(F32)).astype(BF16)
            rs1(b, odd).start()

        def st2(b, odd):
            rs1(b, odd).wait_recv()
            keep = s1_s[b, yy, xx].astype(F32)
            if odd:
                keep = keep + r1_s[b, xx].astype(F32)
                give = s1_s[b, yy, 1 - xx].astype(F32) + r1_s[b, 1 - xx].astype(F32)
            else:
                keep = keep + r1_s[b, yy].astype(F32)
                give = s1_s[b, 1 - yy, xx].astype(F32) + r1_s[b, 1 - yy].astype(F32)
            s2_s[b] = give.astype(BF16)
            rs2(b, odd).start()
            own_s[b] = keep

        def st3(b, odd):
            rs2(b, odd).wait_recv()
            finish(b, own_s[b] + r2_s[b].astype(F32))
            agx(b, odd).start()
            agy(b, odd).start()

            @pl.when(b >= blocks - DIRECT)
            def _():
                far(b, odd).start()

            ags(b, odd).start()

        def st4(b, odd):
            agx(b, odd).wait_recv()
            agy(b, odd).wait_recv()

            @pl.when(b < blocks - DIRECT)
            def _():
                fwd(b, odd).start()

            fxs(b, odd).start()
            fys(b, odd).start()

        def st5(b, odd):
            far(b, odd).wait_recv()
            fds(b, odd).start()

        def st6(b, odd):
            for make in (ags, fxs, fys, fds):
                make(b, odd).wait_recv()

        stages = (st0, st1, st2, st3, st4, st5, st6)

        def drain(low, high):
            @pl.loop(low, high)
            def _(b):
                for make in (d2d, rs1, rs2, agx, agy, ags, far, fxs, fys, fds):
                    make(b, 0).wait_send()

        @pl.loop(0, (blocks + lead[-1] + 1) // 2)
        def _(t):
            for half in range(2):
                for stage, lag in zip(stages, lead):
                    b = 2 * t + half - lag

                    @pl.when((b >= 0) & (b < blocks))
                    def _():
                        stage(b, (half - lag) % 2)
                if extra is not None:
                    extra(2 * t + half, drain)

        drain(0 if extra is None else wides, blocks)

    def put(b, value):
        p_s[b] = value.astype(BF16).reshape(2, 2, 2, part, COLS)

    def att_where(dev, b):
        return pl.ds(pl.multiple_of((b // wides) * side + dev * part, part), part), cols(b % wides)

    def own_rows(h):
        return pl.ds(pl.multiple_of(h * part, part), part)

    def side_rows(h):
        return pl.ds(pl.multiple_of(h * side, side), side)

    def att_block(b):
        @pl.when(b < wides)
        def _():
            wo_copy(b).wait()

        sl = side_rows(b // wides)
        w = wo_s[b % wides].reshape(experts * PAIR, COLS)
        total = None
        for k in range(2):
            prod = jnp.dot(a_s[sl, k * experts * PAIR:(k + 1) * experts * PAIR], w, preferred_element_type=F32)
            prod = prod * jnp.concatenate([g_s[k, sl, :]] * (COLS // 128), axis=1)
            total = prod if total is None else total + prod
        put(b, total)

        @pl.when(b < SLOTS)
        def _():
            for cp in up_copies(b, b):
                cp.start()

        @pl.when((b >= SLOTS) & (b < SLOTS + DSLOTS))
        def _():
            wd_copy(b - SLOTS).start()

    def att_finish(b, total):
        h = own_rows(b // wides)
        row, col = att_where(me, b)
        mid = (xo_s[h, col].astype(F32) + total).astype(BF16)
        xm_s[h, col] = mid
        u_s[row, col] = mid

    here = me.astype(F32)
    lane = lax.broadcasted_iota(jnp.int32, (side, experts), 1).astype(F32)

    def norm_side(h):
        sl = slice(h * side, (h + 1) * side)
        rms_group(u_s, norm_ref, u_s, sl)
        logits = lax.dot_general(u_s[sl, :], router_ref[...], (((1,), (1,)), ((), ())), preferred_element_type=F32)
        id2, id3 = mid_s[0, sl, :], mid_s[1, sl, :]
        l0 = jnp.sum(jnp.where(lane == id2[:, 0:experts], logits, 0.0), axis=1, keepdims=True)
        l1 = jnp.sum(jnp.where(lane == id3[:, 0:experts], logits, 0.0), axis=1, keepdims=True)
        top = jnp.maximum(l0, l1)
        e0, e1 = jnp.exp(l0 - top), jnp.exp(l1 - top)
        inv = 1.0 / (e0 + e1)
        wb_s[sl, :] = jnp.where(id2 == here, e0 * inv, 0.0) + jnp.where(id3 == here, e1 * inv, 0.0)

    def glu(f, slot, sl):
        g = jnp.dot(u_s[sl, :], wg_s[slot], preferred_element_type=F32)
        up = jnp.dot(u_s[sl, :], wu_s[slot], preferred_element_type=F32)
        a_s[sl, pl.ds(pl.multiple_of(f * FB, FB), FB)] = (g * (1.0 / (1.0 + jnp.exp(-g))) * up).astype(BF16)

    att_lead = (0, 1, 3, 5, 7, 9, 11)
    first = wides - 1 + att_lead[-1]

    def early(t, drain):
        @pl.when(t == first)
        def _():
            drain(0, wides)
            norm_side(0)

        f = t - first

        @pl.when((f >= 0) & (f < SLOTS))
        def _():
            for cp in up_copies(f, f):
                cp.wait()
            glu(f, f, slice(0, side))

    all_reduce(0, att_block, att_lead, u_s, att_where, att_finish, early)
    norm_side(1)

    @pl.loop(0, SLOTS)
    def _(f):
        glu(f, f, slice(side, tokens))
        for cp in up_copies(f + SLOTS, f):
            cp.start()

    @pl.loop(SLOTS, fblocks)
    def _(f):
        slot = f % SLOTS
        for cp in up_copies(f, slot):
            cp.wait()
        glu(f, slot, slice(0, tokens))

        @pl.when(f + SLOTS < fblocks)
        def _():
            for cp in up_copies(f + SLOTS, slot):
                cp.start()

    def down_where(dev, b):
        return pl.ds(pl.multiple_of(dev * rows + (b % 2) * part, part), part), cols(b // 2)

    def down_block(b):
        d = b // 2

        @pl.when(b % 2 == 0)
        def _():
            wd_copy(d).wait()

        sl = side_rows(b % 2)
        y = jnp.dot(a_s[sl, :], wd_s[d % DSLOTS], preferred_element_type=F32)
        put(b, y * jnp.concatenate([wb_s[sl, :]] * (COLS // 128), axis=1))

        @pl.when((b % 2 == 1) & (d + DSLOTS < wides))
        def _():
            wd_copy(d + DSLOTS).start()

    def down_finish(b, total):
        row, col = down_where(me, b)
        out_ref[row, col] = (xm_s[own_rows(b % 2), col].astype(F32) + total).astype(BF16)

    all_reduce(1, down_block, (0, 1, 3, 5, 7, 9, 11), out_ref, down_where, down_finish)


def out_mlp(o, ids, mids, gates, x, norm, router, wo, wg, wu, wd):
    tokens, width = x.shape
    experts = wo.shape[0]
    rows = tokens // 8
    part = rows // 2
    blocks = 2 * (width // COLS)
    vmem = pl.BlockSpec(memory_space=pltpu.VMEM)
    hbm = pl.BlockSpec(memory_space=pl.ANY)
    return pl.pallas_call(
        om_kernel,
        name="out_mlp",
        out_shape=pltpu.VMEM((tokens, width), BF16),
        in_specs=[vmem] * 4 + [hbm] + [vmem] * 2 + [hbm] * 4,
        out_specs=vmem,
        scratch_shapes=[
            pltpu.VMEM((width // COLS, experts, wo.shape[1], COLS), BF16),
            pltpu.VMEM((SLOTS, width, FB), BF16), pltpu.VMEM((SLOTS, width, FB), BF16),
            pltpu.VMEM((DSLOTS, wd.shape[0], COLS), BF16),
            pltpu.VMEM((tokens, wd.shape[0]), BF16), pltpu.VMEM((tokens, width), BF16),
            pltpu.VMEM((rows, width), BF16), pltpu.VMEM((rows, width), BF16), pltpu.VMEM((tokens, 128), F32), pltpu.VMEM((2, tokens, 128), F32), pltpu.VMEM((2, tokens, 128), F32),
            pltpu.VMEM((blocks, 2, 2, 2, part, COLS), BF16), pltpu.VMEM((blocks, 2, 2, part, COLS), BF16),
            pltpu.VMEM((blocks, 2, 2, part, COLS), BF16), pltpu.VMEM((blocks, 2, part, COLS), BF16),
            pltpu.VMEM((blocks, part, COLS), F32), pltpu.VMEM((blocks, part, COLS), BF16), pltpu.VMEM((blocks, part, COLS), BF16),
            pltpu.SemaphoreType.DMA((2, 10, blocks)), pltpu.SemaphoreType.DMA((2, 10, blocks)),
            pltpu.SemaphoreType.DMA((width // COLS,)), pltpu.SemaphoreType.DMA((SLOTS,)), pltpu.SemaphoreType.DMA((SLOTS,)),
            pltpu.SemaphoreType.DMA((DSLOTS,)), pltpu.SemaphoreType.DMA],
        compiler_params=pltpu.CompilerParams(vmem_limit_bytes=LIM, collective_id=0, has_side_effects=True),
    )(o, ids, mids, gates, x, norm, router, wo, wg, wu, wd)


def solution(mesh):
    def local_step(x, k_cache, v_cache, positions, att_ids, mlp_ids, norm_att, w_kv, router_att, w_query, w_out, norm_mlp, router_mlp, w_gate, w_up, w_down):
        tokens, width = x.shape
        cache_shape = k_cache.shape
        heads, head_dim = cache_shape[2], cache_shape[3]
        half = np.arange(head_dim // 2, dtype=np.float64)
        freq = (ROPE_BASE ** (-(half * 2.0 / head_dim))).astype(np.float32)
        freq = np.concatenate([freq, freq])[None, :]
        wkv = w_kv.reshape(width, heads, 2, head_dim).transpose(0, 2, 1, 3).reshape(-1, head_dim)
        att, gates, keys_all, values_all = attention(
            positions, att_ids.T, positions[None, :], freq, norm_att[None, :], router_att.T, x, wkv, w_query,
            k_cache.reshape(-1, head_dim), v_cache.reshape(-1, head_dim))
        att = pltpu.with_memory_space_constraint(att, pltpu.VMEM)
        x_out = out_mlp(att, att_ids.T, mlp_ids.T, gates, x, norm_mlp[None, :], router_mlp.T, w_out, w_gate[0], w_up[0], w_down[0])
        return x_out, keys_all.reshape(cache_shape), values_all.reshape(cache_shape)

    token_spec = P('dp', None)
    cache_spec = P('dp', None, 'tp', None)
    expert_spec = P('tp', None, None)
    in_specs = (token_spec, cache_spec, cache_spec, P('dp'), token_spec, token_spec, P(), P(None, 'tp', None), P(), P(None, None, 'tp'), P(None, 'tp', None), P(), P(), expert_spec, expert_spec, expert_spec)
    out_specs = (token_spec, cache_spec, cache_spec)
    return jax.shard_map(local_step, mesh=mesh, in_specs=in_specs, out_specs=out_specs, check_vma=False)
```
